8 devices in a mesh: rep: 1 (over z), dp: 8 (over y, x, core).
Axes of the slice: x: 2, y: 2, z: 1, core: 2. Of those that a mesh axis runs over, the one named last changes fastest.
Arguments:
- hidden: bfloat16 [256, 2048], P(('rep', 'dp'))
- lengths: int32 [256], P(('rep', 'dp'))
- kv_cache: bfloat16 [2, 256, 512, 576], P(None, ('rep', 'dp'))
- norm_attn: float32 [2, 2048], replicated
- w_q: bfloat16 [2, 2048, 9216], replicated
- w_o: bfloat16 [2, 8192, 2048], replicated
- norm_ffn: float32 [2, 2048], replicated
- w_gate: bfloat16 [2, 2048, 10944], P(None, None, 'dp')
- w_up: bfloat16 [2, 2048, 10944], P(None, None, 'dp')
- w_down: bfloat16 [2, 10944, 2048], P(None, 'dp')
- norm_final: float32 [2048], replicated
- w_head: bfloat16 [2048, 102400], P(None, 'dp')
Outputs:
- output: float32 [256, 102400], P('rep', 'dp')
All inputs are finite; a program needn't handle non-finite values.
Results may differ from the reference program's by a relative error of at most 0.02.
Values are sent between devices in bfloat16 or wider.
A program may use at most 1.25 GiB of HBM per device.

```python
import jax
import jax.numpy as jnp
from jax import lax

BATCH_SIZE = 256
SEQ_LEN = 512
D_MODEL = 2048
NUM_HEADS = 16
FFN_DIM = 10944
VOCAB_SIZE = 102400
NUM_LAYERS = 2
LATENT_DIM = 512
ROPE_DIM = 64
KV_WIDTH = LATENT_DIM + ROPE_DIM
QK_SCALE = 192 ** -0.5
NORM_EPS = 1e-6


def setup_inputs(seed: int = 0, part: int = 0) -> dict:
    own_keys = jax.random.split(jax.random.fold_in(jax.random.key(seed), part), 3)
    shared_keys = jax.random.split(jax.random.key(seed + 1), 9)
    hidden = jax.random.normal(own_keys[0], (BATCH_SIZE, D_MODEL), jnp.float32)
    lengths = jax.random.randint(own_keys[1], (BATCH_SIZE,), 1, SEQ_LEN + 1, jnp.int32)
    lengths = lengths.at[0].set(SEQ_LEN)
    kv_cache = jax.random.normal(own_keys[2], (NUM_LAYERS, BATCH_SIZE, SEQ_LEN, KV_WIDTH), jnp.float32)
    attn_gain = SEQ_LEN ** 0.5 / 8.0
    norm_attn = jax.random.uniform(shared_keys[0], (NUM_LAYERS, D_MODEL), jnp.float32, 0.5, 1.5)
    w_q = jax.random.normal(shared_keys[1], (NUM_LAYERS, D_MODEL, NUM_HEADS * KV_WIDTH), jnp.float32) * D_MODEL ** -0.5
    w_o = jax.random.normal(shared_keys[2], (NUM_LAYERS, NUM_HEADS * LATENT_DIM, D_MODEL), jnp.float32) * ((NUM_HEADS * LATENT_DIM) ** -0.5 * attn_gain)
    norm_ffn = jax.random.uniform(shared_keys[3], (NUM_LAYERS, D_MODEL), jnp.float32, 0.5, 1.5)
    w_gate = jax.random.normal(shared_keys[4], (NUM_LAYERS, D_MODEL, FFN_DIM), jnp.float32) * D_MODEL ** -0.5
    w_up = jax.random.normal(shared_keys[5], (NUM_LAYERS, D_MODEL, FFN_DIM), jnp.float32) * D_MODEL ** -0.5
    w_down = jax.random.normal(shared_keys[6], (NUM_LAYERS, FFN_DIM, D_MODEL), jnp.float32) * (2.0 * FFN_DIM ** -0.5)
    norm_final = jax.random.uniform(shared_keys[7], (D_MODEL,), jnp.float32, 0.5, 1.5)
    w_head = jax.random.normal(shared_keys[8], (D_MODEL, VOCAB_SIZE), jnp.float32) * D_MODEL ** -0.5
    return dict(
        hidden=hidden.astype(jnp.bfloat16),
        lengths=lengths,
        kv_cache=kv_cache.astype(jnp.bfloat16),
        norm_attn=norm_attn,
        w_q=w_q.astype(jnp.bfloat16),
        w_o=w_o.astype(jnp.bfloat16),
        norm_ffn=norm_ffn,
        w_gate=w_gate.astype(jnp.bfloat16),
        w_up=w_up.astype(jnp.bfloat16),
        w_down=w_down.astype(jnp.bfloat16),
        norm_final=norm_final,
        w_head=w_head.astype(jnp.bfloat16),
    )


def rms_norm(x_rows, gain_vec):
    x_float = x_rows.astype(jnp.float32)
    inv_rms = lax.rsqrt(jnp.mean(x_float * x_float, axis=-1, keepdims=True) + NORM_EPS)
    return (x_float * inv_rms * gain_vec).astype(jnp.bfloat16)


def attend_row(row_args):
    q_heads, cache_row, length = row_args
    cache_float = cache_row.astype(jnp.float32)
    scores = jnp.dot(q_heads.astype(jnp.float32), cache_float.T, preferred_element_type=jnp.float32) * QK_SCALE
    key_valid = jnp.arange(cache_row.shape[0]) < length
    scores = jnp.where(key_valid[None, :], scores, -1e30)
    attn_probs = jax.nn.softmax(scores, axis=-1).astype(jnp.bfloat16)
    context = jnp.dot(attn_probs.astype(jnp.float32), cache_float[:, :LATENT_DIM], preferred_element_type=jnp.float32)
    return context.astype(jnp.bfloat16)


def reference(hidden, lengths, kv_cache, norm_attn, w_q, w_o, norm_ffn, w_gate, w_up, w_down, norm_final, w_head):
    num_rows = hidden.shape[0]

    def layer_step(x_rows, layer_args):
        layer_cache, attn_norm, wq_layer, wo_layer, ffn_norm, gate_layer, up_layer, down_layer = layer_args
        normed = rms_norm(x_rows, attn_norm)
        q_all = jnp.dot(normed, wq_layer, preferred_element_type=jnp.float32).astype(jnp.bfloat16)
        q_all = q_all.reshape(num_rows, NUM_HEADS, KV_WIDTH)
        context = lax.map(attend_row, (q_all, layer_cache, lengths)).reshape(num_rows, NUM_HEADS * LATENT_DIM)
        x_rows = (x_rows.astype(jnp.float32) + jnp.dot(context, wo_layer, preferred_element_type=jnp.float32)).astype(jnp.bfloat16)
        normed = rms_norm(x_rows, ffn_norm)
        gate_proj = jnp.dot(normed, gate_layer, preferred_element_type=jnp.float32)
        up_proj = jnp.dot(normed, up_layer, preferred_element_type=jnp.float32)
        act_rows = (jax.nn.silu(gate_proj) * up_proj).astype(jnp.bfloat16)
        ffn_out = jnp.dot(act_rows, down_layer, preferred_element_type=jnp.float32)
        x_rows = (x_rows.astype(jnp.float32) + ffn_out).astype(jnp.bfloat16)
        return x_rows, None

    layer_inputs = (kv_cache, norm_attn, w_q, w_o, norm_ffn, w_gate, w_up, w_down)
    x_final, layer_outs = lax.scan(layer_step, hidden, layer_inputs)
    normed = rms_norm(x_final, norm_final)
    return jnp.dot(normed, w_head, preferred_element_type=jnp.float32)
```

```python
import functools

import jax
import jax.numpy as jnp
from jax import lax
from jax.experimental import pallas as pl
from jax.experimental.pallas import tpu as pltpu
from jax.sharding import PartitionSpec as P

LATENT_DIM = 512
QK_SCALE = 192 ** -0.5
NORM_EPS = 1e-6
MESH_ID = pl.DeviceIdType.MESH
NUM_DEV = 8
RS_CHUNK = 512


def rms_norm(x_rows, gain_vec):
    x_float = x_rows.astype(jnp.float32)
    inv_rms = lax.rsqrt(jnp.mean(x_float * x_float, axis=-1, keepdims=True) + NORM_EPS)
    return (x_float * inv_rms * gain_vec).astype(jnp.bfloat16)


def mla_attention(normed, w_q, kv_cache, lengths):
    num_rows, seq_len, kv_width = kv_cache.shape
    q_heads = jnp.dot(normed, w_q, preferred_element_type=jnp.float32).astype(jnp.bfloat16)
    q_heads = q_heads.reshape(num_rows, -1, kv_width)
    scores = jnp.einsum('bhc,btc->bht', q_heads, kv_cache, preferred_element_type=jnp.float32) * QK_SCALE
    key_pos = lax.broadcasted_iota(jnp.int32, (1, 1, seq_len), 2)
    scores = jnp.where(key_pos < lengths[:, None, None], scores, -1e30)
    attn_probs = jax.nn.softmax(scores, axis=-1).astype(jnp.bfloat16)
    context = jnp.einsum('bht,btc->bhc', attn_probs, kv_cache[:, :, :LATENT_DIM], preferred_element_type=jnp.float32)
    return context.astype(jnp.bfloat16).reshape(num_rows, -1)


def add_residual(x_rows, delta):
    return (x_rows.astype(jnp.float32) + delta).astype(jnp.bfloat16)


def ffn_cuts(width):
    return [(lo, min(lo + 512, width)) for lo in range(0, width, 512)]


def peers():
    me = lax.axis_index('dp')
    core, x, y = me % 2, (me // 2) % 2, me // 4
    flip = lambda c, a, b: ((y + b) % 2) * 4 + ((x + a) % 2) * 2 + (core + c) % 2
    return me, {1: flip(1, 0, 0), 2: flip(0, 1, 0), 4: flip(0, 0, 1), 6: flip(0, 1, 1)}


def remote(src, dst, send, recv, dev):
    return pltpu.make_async_remote_copy(src_ref=src, dst_ref=dst, send_sem=send, recv_sem=recv,
                                        device_id={'dp': dev}, device_id_type=MESH_ID)


def ffn_kernel(layer, last, x_ref, gain_ref, gfin_ref, wg_hbm, wu_hbm, wd_hbm, *refs):
    if last:
        (out_ref, rows, wg, wu, wd, act, part, pair_in, total, chip_in, fin,
         w_sem, ag_send, ag_recv, pair_send, pair_recv, chip_send, chip_recv, fin_send, fin_recv) = refs
    else:
        (out_ref, rows, wg, wu, wd, act, part, pair_in, total, chip_in,
         w_sem, ag_send, ag_recv, pair_send, pair_recv, chip_send, chip_recv) = refs
    me, peer = peers()
    n_rows, d_model = x_ref.shape
    width = wg.shape[1]
    cuts = ffn_cuts(width)
    n_cuts, n_chunks = len(cuts), d_model // RS_CHUNK

    loads = []
    for i, (lo, hi) in enumerate(cuts):
        for j, (src, dst) in enumerate(((wg_hbm, wg), (wu_hbm, wu))):
            copy = pltpu.make_async_copy(src.at[layer, :, pl.ds(lo, hi - lo)], dst.at[:, pl.ds(lo, hi - lo)],
                                         w_sem.at[2 * i + j])
            copy.start()
            loads.append(copy)
    down_loads = []
    for c in range(n_chunks):
        cols = pl.ds(c * RS_CHUNK, RS_CHUNK)
        copy = pltpu.make_async_copy(wd_hbm.at[layer, :, cols], wd.at[:, cols], w_sem.at[2 * n_cuts + c])
        copy.start()
        down_loads.append(copy)

    rows[0] = rms_norm(x_ref[...], gain_ref[...])

    barrier = pltpu.get_barrier_semaphore()
    for j in (1, 2, 4, 6):
        pl.semaphore_signal(barrier, inc=1, device_id={'dp': peer[j]}, device_id_type=MESH_ID)
    pl.semaphore_wait(barrier, 4)

    sends = {j: remote(rows.at[0], rows.at[j], ag_send.at[j], ag_recv.at[j], peer[j]) for j in (6, 2, 4, 1)}
    for copy in sends.values():
        copy.start()
    for j in (2, 4, 6):
        sends[j].wait_recv()
        sends[j + 1] = remote(rows.at[j], rows.at[j + 1], ag_send.at[j + 1], ag_recv.at[j + 1], peer[1])
        sends[j + 1].start()
    for j in (1, 3, 5, 7):
        sends[j].wait_recv()

    for i, (lo, hi) in enumerate(cuts):
        cols = pl.ds(lo, hi - lo)
        loads[2 * i].wait()
        loads[2 * i + 1].wait()
        full = rows[...].reshape(NUM_DEV * n_rows, d_model)
        gate = jnp.dot(full, wg[:, cols], preferred_element_type=jnp.float32)
        up = jnp.dot(full, wu[:, cols], preferred_element_type=jnp.float32)
        act[:, cols] = (jax.nn.silu(gate) * up).astype(jnp.bfloat16)

    pair, chip = [], []

    def reduce_chunk(c):
        pair[c].wait_recv()
        for k in range(4):
            both = part[c, k, 0] + pair_in[c, k]
            if k == 0:
                part[c, 0, 0] = both
            else:
                total[c, k - 1] = both.astype(jnp.bfloat16)
        for k in (3, 1, 2):
            copy = remote(total.at[c, k - 1], chip_in.at[c, k - 1], chip_send.at[c, k - 1], chip_recv.at[c, k - 1],
                          peer[2 * k])
            copy.start()
            chip.append(copy)

    for c in range(n_chunks):
        down_loads[c].wait()
        y = jnp.dot(act[...], wd[:, pl.ds(c * RS_CHUNK, RS_CHUNK)], preferred_element_type=jnp.float32)
        part[c] = y.reshape(4, 2, n_rows, RS_CHUNK)
        copy = remote(part.at[c, :, 1], pair_in.at[c], pair_send.at[c], pair_recv.at[c], peer[1])
        copy.start()
        pair.append(copy)
        if c >= 1:
            reduce_chunk(c - 1)
    reduce_chunk(n_chunks - 1)

    for copy in chip:
        copy.wait_recv()
    x_new = []
    for c in range(n_chunks):
        cols = pl.ds(c * RS_CHUNK, RS_CHUNK)
        y = part[c, 0, 0]
        for k in range(3):
            y = y + chip_in[c, k].astype(jnp.float32)
        x_new.append((x_ref[:, cols].astype(jnp.float32) + y).astype(jnp.bfloat16))
    x_new = jnp.concatenate(x_new, axis=1)

    if last:
        fin[...] = rms_norm(x_new, gfin_ref[...])
        out_ref[me] = fin[...]
    else:
        out_ref[...] = x_new

    for copy in list(sends.values()) + pair + chip:
        copy.wait_send()

    if last:
        own = out_ref.at[me]
        sends = {j: remote(fin, own, fin_send.at[j], fin_recv.at[j], peer[j]) for j in (6, 2, 4, 1)}
        for copy in sends.values():
            copy.start()
        for j in (2, 4, 6):
            sends[j].wait_recv()
            theirs = out_ref.at[peer[j]]
            sends[j + 1] = remote(theirs, theirs, fin_send.at[j + 1], fin_recv.at[j + 1], peer[1])
            sends[j + 1].start()
        for j in (1, 3, 5, 7):
            sends[j].wait_recv()
        for copy in sends.values():
            copy.wait_send()


def ffn_layer(layer, last, x_rows, gain, gain_final, w_gate, w_up, w_down):
    n_rows, d_model = x_rows.shape
    width = w_gate.shape[2]
    n_chunks = d_model // RS_CHUNK
    n_w = 2 * len(ffn_cuts(width)) + n_chunks
    vmem, any_space = pl.BlockSpec(memory_space=pltpu.VMEM), pl.BlockSpec(memory_space=pl.ANY)
    bf16, f32, dma = jnp.bfloat16, jnp.float32, pltpu.SemaphoreType.DMA
    scratch = [
        pltpu.VMEM((NUM_DEV, n_rows, d_model), bf16),
        pltpu.VMEM((d_model, width), bf16),
        pltpu.VMEM((d_model, width), bf16),
        pltpu.VMEM((width, d_model), bf16),
        pltpu.VMEM((NUM_DEV * n_rows, width), bf16),
        pltpu.VMEM((n_chunks, 4, 2, n_rows, RS_CHUNK), f32),
        pltpu.VMEM((n_chunks, 4, n_rows, RS_CHUNK), f32),
        pltpu.VMEM((n_chunks, 3, n_rows, RS_CHUNK), bf16),
        pltpu.VMEM((n_chunks, 3, n_rows, RS_CHUNK), bf16),
    ]
    if last:
        scratch.append(pltpu.VMEM((n_rows, d_model), bf16))
    scratch += [dma((n_w,)), dma((8,)), dma((8,)), dma((n_chunks,)), dma((n_chunks,)), dma((n_chunks, 3)), dma((n_chunks, 3))]
    if last:
        scratch += [dma((8,)), dma((8,))]
    out_shape = (NUM_DEV, n_rows, d_model) if last else (n_rows, d_model)
    return pl.pallas_call(
        functools.partial(ffn_kernel, layer, last),
        out_shape=jax.ShapeDtypeStruct(out_shape, bf16),
        in_specs=[vmem, vmem, vmem, any_space, any_space, any_space],
        out_specs=vmem,
        scratch_shapes=scratch,
        compiler_params=pltpu.CompilerParams(collective_id=layer, has_side_effects=True,
                                             vmem_limit_bytes=48 * 1024 * 1024),
        name=f'ffn{layer}',
    )(x_rows, gain.reshape(1, -1), gain_final.reshape(1, -1), w_gate, w_up, w_down)


def solution(mesh):
    row_axes = ('rep', 'dp')
    specs_in = (P(row_axes, None), P(row_axes), P(None, row_axes, None, None), P(), P(), P(), P(),
                P(None, None, 'dp'), P(None, None, 'dp'), P(None, 'dp', None), P(), P(None, 'dp'))

    def device_step(hidden, lengths, kv_cache, norm_attn, w_q, w_o, norm_ffn, w_gate, w_up, w_down, norm_final, w_head):
        x_rows = hidden
        num_layers = kv_cache.shape[0]
        for layer_idx in range(num_layers):
            normed = rms_norm(x_rows, norm_attn[layer_idx])
            context = mla_attention(normed, w_q[layer_idx], kv_cache[layer_idx], lengths)
            x_rows = add_residual(x_rows, jnp.dot(context, w_o[layer_idx], preferred_element_type=jnp.float32))
            x_rows = ffn_layer(layer_idx, layer_idx == num_layers - 1, x_rows, norm_ffn[layer_idx], norm_final,
                               w_gate, w_up, w_down)
        gathered = x_rows.reshape(-1, hidden.shape[1])
        return jnp.dot(gathered, w_head, preferred_element_type=jnp.float32)

    return jax.shard_map(device_step, mesh=mesh, in_specs=specs_in, out_specs=P('rep', 'dp'), check_vma=False)
```

```python
import functools

import jax
import jax.numpy as jnp
from jax import lax
from jax.experimental import pallas as pl
from jax.experimental.pallas import tpu as pltpu
from jax.sharding import PartitionSpec as P

LATENT = 512
QK_SCALE = 192 ** -0.5
NORM_EPS = 1e-6
MESH_ID = pl.DeviceIdType.MESH
NUM_DEV = 8
CHUNK = 512
GROUP = 4
BF16, F32 = jnp.bfloat16, jnp.float32


def rms_norm(x_rows, gain_vec):
    x_float = x_rows.astype(F32)
    inv_rms = lax.rsqrt(jnp.mean(x_float * x_float, axis=-1, keepdims=True) + NORM_EPS)
    return (x_float * inv_rms * gain_vec).astype(BF16)


def dot(a, b):
    return jnp.dot(a, b, preferred_element_type=F32)


def dot_nt(a, b):
    return lax.dot_general(a, b, (((1,), (1,)), ((), ())), preferred_element_type=F32)


def round_up(n, m):
    return (n + m - 1) // m * m


def cuts_of(width):
    return [(lo, min(lo + CHUNK, width)) for lo in range(0, width, CHUNK)]


def layers_kernel(dims, x_ref, len_ref, gain_attn, gain_ffn, gain_fin, kv_hbm, wq_hbm, wo_hbm, wg_hbm, wu_hbm, wd_hbm,
                  rows, buf, x_cur, hrows, qo, qsend, p_buf, ol, ol_send, ps, pr, act, pair_send, pair_in, total, chip_in,
                  fin, wq_sem, kv_sem, wo_sem, ffn_sem, h_sem, q_sem, o_sem, p_sem, ag_sem, pair_sem, chip_sem, fin_sem):
    n_layers, n_rows, d_model, n_heads, kv_width, seq_len, width, pad_width = dims
    half = n_heads // 2
    q_cols = half * kv_width
    n_q, n_d = q_cols // CHUNK, d_model // CHUNK
    o_rows = half * LATENT
    n_t = round_up(kv_width, 128) // 128
    cuts = cuts_of(width)

    me = lax.axis_index('dp')
    core, x_pos, y_pos = me % 2, (me // 2) % 2, me // 4
    flip = lambda c, a, b: ((y_pos + b) % 2) * 4 + ((x_pos + a) % 2) * 2 + (core + c) % 2
    peer = {1: flip(1, 0, 0), 2: flip(0, 1, 0), 4: flip(0, 0, 1), 6: flip(0, 1, 1)}
    other = 1 - core

    def remote(src, dst, sems, dev):
        return pltpu.make_async_remote_copy(src_ref=src, dst_ref=dst, send_sem=sems.at[0], recv_sem=sems.at[1],
                                            device_id={'dp': dev}, device_id_type=MESH_ID)

    wq_buf = lambda l: l % 3
    kv_buf = lambda l: (l + 1) % 3
    wo_buf = lambda l: (l + 2) % 3
    ffn_buf = wq_buf

    def wq_copy(l, n):
        cols = pl.ds(pl.multiple_of(core * q_cols + n * CHUNK, 128), CHUNK)
        return pltpu.make_async_copy(wq_hbm.at[l, :, cols], buf.at[wq_buf(l), pl.ds(n * d_model, d_model)], wq_sem.at[l, n])

    def kv_copy(l, b):
        row = b * kv_width if isinstance(b, int) else pl.multiple_of(b * kv_width, 64)
        return pltpu.make_async_copy(kv_hbm.at[l, b], buf.at[kv_buf(l), pl.ds(row, kv_width)], kv_sem.at[l, b])

    def wo_copy(l, n):
        src = wo_hbm.at[l, pl.ds(pl.multiple_of(core * o_rows, 128), o_rows), pl.ds(n * CHUNK, CHUNK)]
        return pltpu.make_async_copy(src, buf.at[wo_buf(l), pl.ds(n * o_rows, o_rows)], wo_sem.at[l, n])

    def ffn_copy(l, i):
        src = (wg_hbm, wu_hbm, wd_hbm)[i // n_d]
        return pltpu.make_async_copy(src.at[l, :, pl.ds((i % n_d) * CHUNK, CHUNK)],
                                     buf.at[ffn_buf(l), pl.ds(i * pad_width, width)], ffn_sem.at[l, i])

    def start(copies):
        for copy in copies:
            copy.start()

    def gather(own, slot_of, sems):
        sends = {j: remote(own, slot_of(0, j), sems.at[j], peer[j]) for j in (6, 2, 4, 1)}
        start(sends.values())
        for j in (2, 4, 6):
            sends[j].wait_recv()
            sends[j + 1] = remote(slot_of(j, j), slot_of(j, j + 1), sems.at[j + 1], peer[1])
            sends[j + 1].start()
        for j in (1, 3, 5, 7):
            sends[j].wait_recv()
        return list(sends.values())

    start(wq_copy(0, n) for n in range(n_q))
    x_cur[...] = x_ref[...]

    for l in range(n_layers):
        sent = []
        hrows[0] = rms_norm(x_cur[...], gain_attn[pl.ds(l, 1), :])
        if l == 0:
            barrier = pltpu.get_barrier_semaphore()
            for j in (1, 2, 4, 6):
                pl.semaphore_signal(barrier, inc=1, device_id={'dp': peer[j]}, device_id_type=MESH_ID)
            pl.semaphore_wait(barrier, 4)
        copy = remote(hrows.at[0], hrows.at[1], h_sem.at[l], peer[1])
        copy.start()
        sent.append(copy)
        copy.wait_recv()
        both_rows = hrows[...].reshape(2 * n_rows, d_model)
        prev, q_copies = None, []
        for n in range(n_q):
            wq_copy(l, n).wait()
            if l == 0:
                per = -(-n_rows // n_q)
                start(kv_copy(l, b) for b in range(n * per, min((n + 1) * per, n_rows)))
            cur = dot(both_rows, buf[wq_buf(l), pl.ds(n * d_model, d_model), :]).astype(BF16).astype(F32)
            if n >= 1:
                h = n - 1
                off = h * kv_width - h * CHUNK
                q_head = jnp.concatenate([prev[:, off:], cur[:, :off + kv_width - CHUNK]], axis=1)
                for j in range(n_t):
                    lanes = slice(j * 128, min((j + 1) * 128, kv_width))
                    keep = pl.ds(0, lanes.stop - lanes.start)
                    qo[j, pl.ds(pl.multiple_of((core * half + h) * n_rows, n_rows), n_rows), keep] = q_head[:n_rows, lanes]
                    qsend[j, pl.ds(h * n_rows, n_rows), keep] = q_head[n_rows:, lanes]
                if h % 2:
                    dst = qo.at[:, pl.ds(pl.multiple_of((core * half + h - 1) * n_rows, n_rows), 2 * n_rows)]
                    copy = remote(qsend.at[:, pl.ds((h - 1) * n_rows, 2 * n_rows)], dst, q_sem.at[l, h // 2], peer[1])
                    copy.start()
                    q_copies.append(copy)
            prev = cur
        if l == 0:
            start(wo_copy(l, n) for n in range(n_d))
        sent += q_copies
        for copy in q_copies:
            copy.wait_recv()

        key_pos = lax.broadcasted_iota(jnp.int32, (n_heads, seq_len), 1)

        def scores(g, l=l):
            slot = lax.rem(g, 2)
            for i in range(GROUP):
                b = g * GROUP + i
                kv_copy(l, b).wait()
                q = [qo[j, pl.ds(b, n_heads, stride=n_rows), :].astype(BF16) for j in range(n_t)]
                q = jnp.concatenate(q, axis=1)[:, :kv_width]
                row = pl.multiple_of(b * kv_width, 64)
                s = dot(q, buf[kv_buf(l), pl.ds(row, kv_width), :]) * QK_SCALE
                s = jnp.where(key_pos < len_ref[b], s, -1e30)
                e = jnp.exp(s - jnp.max(s, axis=-1, keepdims=True))
                p_buf[slot, i] = (e / jnp.sum(e, axis=-1, keepdims=True)).astype(BF16)

        def contexts(g, l=l):
            slot = lax.rem(g, 2)
            for i in range(GROUP):
                b = g * GROUP + i
                row = pl.multiple_of(b * kv_width, 64)
                ctx = dot_nt(p_buf[slot, i], buf[kv_buf(l), pl.ds(row, LATENT), :])
                for j in range(LATENT // 128):
                    qo[j, pl.ds(b, n_heads, stride=n_rows), :] = ctx[:, j * 128:(j + 1) * 128]

        n_groups = n_rows // GROUP
        scores(jnp.int32(0))

        def step(g, carry):
            scores(g)
            contexts(g - 1)
            return carry

        lax.fori_loop(1, n_groups, step, 0)
        contexts(jnp.int32(n_groups - 1))

        for h in range(half):
            at = pl.ds(pl.multiple_of((other * half + h) * n_rows, n_rows), n_rows)
            for j in range(LATENT // 128):
                ol_send[h, :, pl.ds(j * 128, 128)] = qo[j, at, :].astype(BF16)
        o_copy = remote(ol_send, ol.at[1], o_sem.at[l], peer[1])
        o_copy.start()
        sent.append(o_copy)
        start(ffn_copy(l, i) for i in range(3 * n_d))
        for h in range(half):
            at = pl.ds(pl.multiple_of((core * half + h) * n_rows, n_rows), n_rows)
            for j in range(LATENT // 128):
                ol[0, h, :, pl.ds(j * 128, 128)] = qo[j, at, :].astype(BF16)
        o_copy.wait_recv()
        p_copies, own = [], []
        for n in range(n_d):
            wo_copy(l, n).wait()
            acc = None
            for h in range(half):
                part = dot(ol[:, h].reshape(2 * n_rows, LATENT), buf[wo_buf(l), pl.ds(n * o_rows + h * LATENT, LATENT), :])
                acc = part if acc is None else acc + part
            own.append(acc[:n_rows])
            ps[n] = acc[n_rows:]
            copy = remote(ps.at[n], pr.at[n], p_sem.at[l, n], peer[1])
            copy.start()
            p_copies.append(copy)
        sent += p_copies
        for n in range(n_d):
            cols = pl.ds(n * CHUNK, CHUNK)
            p_copies[n].wait_recv()
            x_cur[:, cols] = (x_cur[:, cols].astype(F32) + (own[n] + pr[n])).astype(BF16)

        rows[0] = rms_norm(x_cur[...], gain_ffn[pl.ds(l, 1), :])
        row_sends = gather(rows.at[0], lambda j, k: rows.at[k], ag_sem.at[l])
        if l + 1 < n_layers:
            start(wq_copy(l + 1, n) for n in range(n_q))
        for i in range(2 * n_d):
            ffn_copy(l, i).wait()
        for lo, hi in cuts:
            gate = up = None
            for k in range(n_d):
                cols = rows[:, :, pl.ds(k * CHUNK, CHUNK)].reshape(NUM_DEV * n_rows, CHUNK)
                g_part = dot_nt(cols, buf[ffn_buf(l), pl.ds(k * pad_width + lo, hi - lo), :])
                u_part = dot_nt(cols, buf[ffn_buf(l), pl.ds((n_d + k) * pad_width + lo, hi - lo), :])
                gate = g_part if gate is None else gate + g_part
                up = u_part if up is None else up + u_part
            act[:, pl.ds(lo, hi - lo)] = (jax.nn.silu(gate) * up).astype(BF16)

        for copy in row_sends:
            copy.wait_send()
        pair, chip = [], []

        def reduce_chunk(c):
            pair[c].wait_recv()
            for k in range(4):
                at = pl.ds((c * 4 + k) * n_rows, n_rows)
                for j in range(CHUNK // 128):
                    lanes = pl.ds(j * 128, 128)
                    both = qo[j, at, :] + pair_in[c, k, :, lanes]
                    if k == 0:
                        qo[j, at, :] = both
                    else:
                        total[c, k - 1, :, lanes] = both.astype(BF16)
            for k in (3, 1, 2):
                copy = remote(total.at[c, k - 1], chip_in.at[c, k - 1], chip_sem.at[l, c, k - 1], peer[2 * k])
                copy.start()
                chip.append(copy)

        for c in range(n_d):
            ffn_copy(l, 2 * n_d + c).wait()
            y = dot(act[...], buf[ffn_buf(l), pl.ds((2 * n_d + c) * pad_width, width), :])
            y = y.reshape(4, 2, n_rows, CHUNK)
            pair_send[c] = y[:, 1]
            mine = y[:, 0].reshape(4 * n_rows, CHUNK)
            for j in range(CHUNK // 128):
                qo[j, pl.ds(c * 4 * n_rows, 4 * n_rows), :] = mine[:, j * 128:(j + 1) * 128]
            copy = remote(pair_send.at[c], pair_in.at[c], pair_sem.at[l, c], peer[1])
            copy.start()
            pair.append(copy)
            if c >= 1:
                reduce_chunk(c - 1)
        reduce_chunk(n_d - 1)
        if l + 1 < n_layers:
            start(kv_copy(l + 1, b) for b in range(n_rows))
            start(wo_copy(l + 1, n) for n in range(n_d))
        for copy in chip:
            copy.wait_recv()
        for c in range(n_d):
            cols = pl.ds(c * CHUNK, CHUNK)
            y = jnp.concatenate([qo[j, pl.ds(c * 4 * n_rows, n_rows), :] for j in range(CHUNK // 128)], axis=1)
            for k in range(3):
                y = y + chip_in[c, k].astype(F32)
            x_cur[:, cols] = (x_cur[:, cols].astype(F32) + y).astype(BF16)
        for copy in sent + pair + chip:
            copy.wait_send()

    fin[...] = rms_norm(x_cur[...], gain_fin[...])
    rows[me] = fin[...]
    peer[0] = me
    sends = gather(fin, lambda j, k: rows.at[peer[j]], fin_sem)
    for copy in sends:
        copy.wait_send()


def run_layers(hidden, lengths, kv_t, gain_attn, w_q, w_o, gain_ffn, wg_t, wu_t, w_down, gain_fin):
    n_layers, n_rows, kv_width, seq_len = kv_t.shape
    d_model = hidden.shape[1]
    n_heads = w_q.shape[2] // kv_width
    width = w_down.shape[1]
    pad_width = round_up(width, 16)
    half, n_d = n_heads // 2, d_model // CHUNK
    n_q = half * kv_width // CHUNK
    n_t = round_up(kv_width, 128) // 128
    buf_rows = max(n_q * d_model, n_rows * kv_width, n_d * half * LATENT, 3 * n_d * pad_width)
    dims = (n_layers, n_rows, d_model, n_heads, kv_width, seq_len, width, pad_width)
    vmem, anys = pl.BlockSpec(memory_space=pltpu.VMEM), pl.BlockSpec(memory_space=pl.ANY)
    smem = pl.BlockSpec(memory_space=pltpu.SMEM)
    dma = pltpu.SemaphoreType.DMA
    scratch = [
        pltpu.VMEM((3, buf_rows, CHUNK), BF16),
        pltpu.VMEM((n_rows, d_model), BF16),
        pltpu.VMEM((2, n_rows, d_model), BF16),
        pltpu.VMEM((n_t, n_heads * n_rows, 128), F32),
        pltpu.VMEM((n_t, half * n_rows, 128), F32),
        pltpu.VMEM((2, GROUP, n_heads, seq_len), BF16),
        pltpu.VMEM((2, half, n_rows, LATENT), BF16),
        pltpu.VMEM((half, n_rows, LATENT), BF16),
        pltpu.VMEM((n_d, n_rows, CHUNK), F32),
        pltpu.VMEM((n_d, n_rows, CHUNK), F32),
        pltpu.VMEM((NUM_DEV * n_rows, width), BF16),
        pltpu.VMEM((n_d, 4, n_rows, CHUNK), F32),
        pltpu.VMEM((n_d, 4, n_rows, CHUNK), F32),
        pltpu.VMEM((n_d, 3, n_rows, CHUNK), BF16),
        pltpu.VMEM((n_d, 3, n_rows, CHUNK), BF16),
        pltpu.VMEM((n_rows, d_model), BF16),
        dma((n_layers, n_q)), dma((n_layers, n_rows)), dma((n_layers, n_d)), dma((n_layers, 3 * n_d)),
        dma((n_layers, 2)), dma((n_layers, half // 2, 2)), dma((n_layers, 2)), dma((n_layers, n_d, 2)),
        dma((n_layers, 8, 2)), dma((n_layers, n_d, 2)), dma((n_layers, n_d, 3, 2)), dma((8, 2)),
    ]
    return pl.pallas_call(
        functools.partial(layers_kernel, dims),
        out_shape=jax.ShapeDtypeStruct((NUM_DEV, n_rows, d_model), BF16),
        in_specs=[vmem, smem, vmem, vmem, vmem] + [anys] * 6,
        out_specs=vmem,
        scratch_shapes=scratch,
        compiler_params=pltpu.CompilerParams(collective_id=0, has_side_effects=True, vmem_limit_bytes=67043328),
        name='layers',
    )(hidden, lengths, gain_attn, gain_ffn, gain_fin.reshape(1, -1), kv_t, w_q, w_o, wg_t, wu_t, w_down)


def solution(mesh):
    row_axes = ('rep', 'dp')
    specs_in = (P(row_axes, None), P(row_axes), P(None, row_axes, None, None), P(), P(), P(), P(),
                P(None, None, 'dp'), P(None, None, 'dp'), P(None, 'dp', None), P(), P(None, 'dp'))

    def device_step(hidden, lengths, kv_cache, norm_attn, w_q, w_o, norm_ffn, w_gate, w_up, w_down, norm_final, w_head):
        gathered = run_layers(hidden, lengths, jnp.swapaxes(kv_cache, 2, 3), norm_attn, w_q, w_o, norm_ffn,
                              jnp.swapaxes(w_gate, 1, 2), jnp.swapaxes(w_up, 1, 2), w_down, norm_final)
        return dot(gathered.reshape(-1, hidden.shape[1]), w_head)

    return jax.shard_map(device_step, mesh=mesh, in_specs=specs_in, out_specs=P('rep', 'dp'), check_vma=False)
```

```python
import functools

import jax
import jax.numpy as jnp
from jax import lax
from jax.experimental import pallas as pl
from jax.experimental.pallas import tpu as pltpu
from jax.sharding import PartitionSpec as P

LATENT = 512
QK_SCALE = 192 ** -0.5
NORM_EPS = 1e-6
MESH_ID = pl.DeviceIdType.MESH
NUM_DEV = 8
CHUNK = 512
GROUP = 8
HEAD_A, HEAD_B = 16, 9
VMEM_LAYERS = int(8.9 * 2**20)
BF16, F32 = jnp.bfloat16, jnp.float32


def rms_norm(x_rows, gain_vec):
    x_float = x_rows.astype(F32)
    inv_rms = lax.rsqrt(jnp.mean(x_float * x_float, axis=-1, keepdims=True) + NORM_EPS)
    return (x_float * inv_rms * gain_vec).astype(BF16)


def dot(a, b):
    return jnp.dot(a, b, preferred_element_type=F32)


def dot_nt(a, b):
    return lax.dot_general(a, b, (((1,), (1,)), ((), ())), preferred_element_type=F32)


def round_up(n, m):
    return (n + m - 1) // m * m


def head_chunk(i):
    return i + i // HEAD_A * 2


def cuts_of(width):
    return [(lo, min(lo + CHUNK, width)) for lo in range(0, width, CHUNK)]


def layers_kernel(dims, x_ref, len_ref, gain_attn, gain_ffn, gain_fin, kv_hbm, wq_hbm, wo_hbm, wg_hbm, wu_hbm, wd_hbm,
                  wh_hbm, rows, buf, x_cur, hrows, qo, outbox, p_buf, ol, ol_send, pr, act, pair_in, total, chip_in,
                  wq_sem, kv_sem, wo_sem, ffn_sem, h_sem, q_sem, o_sem, p_sem, ag_sem, pair_sem, chip_sem, fin_sem, head_sem):
    n_layers, n_rows, d_model, n_heads, kv_width, seq_len, width, pad_width, slot_rows, vocab = dims
    half = n_heads // 2
    q_cols = half * kv_width
    n_q, n_d = q_cols // CHUNK, d_model // CHUNK
    o_rows = half * LATENT
    n_t, n_j = round_up(kv_width, 128) // 128, CHUNK // 128
    cuts = cuts_of(width)
    n_vocab = vocab // CHUNK

    me = lax.axis_index('dp')
    core, x_pos, y_pos = me % 2, (me // 2) % 2, me // 4
    flip = lambda c, a, b: ((y_pos + b) % 2) * 4 + ((x_pos + a) % 2) * 2 + (core + c) % 2
    peer = {1: flip(1, 0, 0), 2: flip(0, 1, 0), 4: flip(0, 0, 1), 6: flip(0, 1, 1)}
    other = 1 - core

    def remote(src, dst, sems, dev):
        return pltpu.make_async_remote_copy(src_ref=src, dst_ref=dst, send_sem=sems.at[0], recv_sem=sems.at[1],
                                            device_id={'dp': dev}, device_id_type=MESH_ID)

    wq_at = lambda l, row, n: pl.ds(l % 3 * slot_rows + row, n)
    kv_at = lambda l, row, n: pl.ds((l + 1) % 3 * slot_rows + row, n)
    wo_at = lambda l, row, n: pl.ds((l + 2) % 3 * slot_rows + row, n)
    ffn_at = wq_at

    def wq_copy(l, n):
        cols = pl.ds(pl.multiple_of(core * q_cols + n * CHUNK, 128), CHUNK)
        return pltpu.make_async_copy(wq_hbm.at[l, :, cols], buf.at[wq_at(l, n * d_model, d_model)], wq_sem.at[l, n])

    def kv_copy(l, b):
        row = b * kv_width if isinstance(b, int) else pl.multiple_of(b * kv_width, 64)
        return pltpu.make_async_copy(kv_hbm.at[l, b], buf.at[kv_at(l, row, kv_width)], kv_sem.at[l, b])

    def wo_copy(l, n):
        src = wo_hbm.at[l, pl.ds(pl.multiple_of(core * o_rows, 128), o_rows), pl.ds(n * CHUNK, CHUNK)]
        return pltpu.make_async_copy(src, buf.at[wo_at(l, n * o_rows, o_rows)], wo_sem.at[l, n])

    def ffn_copy(l, i):
        src = (wg_hbm, wu_hbm, wd_hbm)[i // n_d]
        return pltpu.make_async_copy(src.at[l, :, pl.ds((i % n_d) * CHUNK, CHUNK)],
                                     buf.at[ffn_at(l, i * pad_width, width)], ffn_sem.at[l, i])

    def head_copy(i):
        row = head_chunk(i) * d_model
        return pltpu.make_async_copy(wh_hbm.at[:, pl.ds(i * CHUNK, CHUNK)], buf.at[pl.ds(row, d_model)], head_sem.at[i])

    def start(copies):
        for copy in copies:
            copy.start()

    def gather(own, slot_of, sems):
        sends = {j: remote(own, slot_of(0, j), sems.at[j], peer[j]) for j in (6, 2, 4, 1)}
        start(sends.values())
        for j in (2, 4, 6):
            sends[j].wait_recv()
            sends[j + 1] = remote(slot_of(j, j), slot_of(j, j + 1), sems.at[j + 1], peer[1])
            sends[j + 1].start()
        for j in (1, 3, 5, 7):
            sends[j].wait_recv()
        return list(sends.values())

    start(wq_copy(0, n) for n in range(n_q))
    x_cur[...] = x_ref[...]

    for l in range(n_layers):
        sent = []
        hrows[0] = rms_norm(x_cur[...], gain_attn[pl.ds(l, 1), :])
        if l == 0:
            barrier = pltpu.get_barrier_semaphore()
            for j in (1, 2, 4, 6):
                pl.semaphore_signal(barrier, inc=1, device_id={'dp': peer[j]}, device_id_type=MESH_ID)
            pl.semaphore_wait(barrier, 4)
        copy = remote(hrows.at[0], hrows.at[1], h_sem.at[l], peer[1])
        copy.start()
        sent.append(copy)
        copy.wait_recv()
        both_rows = hrows[...].reshape(2 * n_rows, d_model)
        prev, q_copies = None, []
        for first in range(0, n_q, 3):
            for n in range(first, first + 3):
                wq_copy(l, n).wait()
            if l == 0:
                per = -(-3 * n_rows // n_q)
                start(kv_copy(l, b) for b in range(first // 3 * per, min((first // 3 + 1) * per, n_rows)))
            weights = jnp.concatenate([buf[wq_at(l, n * d_model, d_model), :] for n in range(first, first + 3)], axis=1)
            wide = dot(both_rows, weights).astype(BF16).astype(F32)
            for n in range(first, first + 3):
                cur = wide[:, (n - first) * CHUNK:(n - first + 1) * CHUNK]
                if n >= 1:
                    h = n - 1
                    off = h * kv_width - h * CHUNK
                    q_head = jnp.concatenate([prev[:, off:], cur[:, :off + kv_width - CHUNK]], axis=1)
                    for j in range(n_t):
                        lanes = slice(j * 128, min((j + 1) * 128, kv_width))
                        keep = pl.ds(0, lanes.stop - lanes.start)
                        at = pl.ds(pl.multiple_of((core * half + h) * n_rows, n_rows), n_rows)
                        qo[j, at, keep] = q_head[:n_rows, lanes]
                        outbox[j, pl.ds(h * n_rows, n_rows), keep] = q_head[n_rows:, lanes]
                    if h % 2:
                        dst = qo.at[:, pl.ds(pl.multiple_of((core * half + h - 1) * n_rows, n_rows), 2 * n_rows)]
                        copy = remote(outbox.at[pl.ds(0, n_t), pl.ds((h - 1) * n_rows, 2 * n_rows)], dst, q_sem.at[l, h // 2], peer[1])
                        copy.start()
                        q_copies.append(copy)
                prev = cur
        if l == 0:
            start(wo_copy(l, n) for n in range(n_d))
        for copy in q_copies:
            copy.wait_recv()

        key_pos = lax.broadcasted_iota(jnp.int32, (n_heads, seq_len), 1)

        def scores(g, l=l):
            slot = lax.rem(g, 2)
            for i in range(GROUP):
                kv_copy(l, g * GROUP + i).wait()
            for i in range(GROUP):
                b = g * GROUP + i
                q = [qo[j, pl.ds(b, n_heads, stride=n_rows), :].astype(BF16) for j in range(n_t)]
                q = jnp.concatenate(q, axis=1)[:, :kv_width]
                row = pl.multiple_of(b * kv_width, 64)
                s = dot(q, buf[kv_at(l, row, kv_width), :]) * QK_SCALE
                s = jnp.where(key_pos < len_ref[b], s, -1e30)
                e = jnp.exp(s - jnp.max(s, axis=-1, keepdims=True))
                p_buf[slot, i] = (e / jnp.sum(e, axis=-1, keepdims=True)).astype(BF16)

        def contexts(g, l=l):
            slot = lax.rem(g, 2)
            for i in range(GROUP):
                b = g * GROUP + i
                row = pl.multiple_of(b * kv_width, 64)
                ctx = dot_nt(p_buf[slot, i], buf[kv_at(l, row, LATENT), :])
                for j in range(n_j):
                    qo[j, pl.ds(b, n_heads, stride=n_rows), :] = ctx[:, j * 128:(j + 1) * 128]

        n_groups = n_rows // GROUP
        scores(jnp.int32(0))

        def step(g, carry):
            scores(g)
            contexts(g - 1)
            return carry

        lax.fori_loop(1, n_groups, step, 0)
        contexts(jnp.int32(n_groups - 1))
        if l + 1 == n_layers:
            start(head_copy(i) for i in range(HEAD_A, n_vocab))

        for copy in q_copies:
            copy.wait_send()

        for h in range(half):
            at = pl.ds(pl.multiple_of((other * half + h) * n_rows, n_rows), n_rows)
            for j in range(n_j):
                ol_send[h, :, pl.ds(j * 128, 128)] = qo[j, at, :].astype(BF16)
        o_copy = remote(ol_send, ol.at[1], o_sem.at[l], peer[1])
        o_copy.start()
        sent.append(o_copy)
        start(ffn_copy(l, i) for i in range(3 * n_d))
        for h in range(half):
            at = pl.ds(pl.multiple_of((core * half + h) * n_rows, n_rows), n_rows)
            for j in range(n_j):
                ol[0, h, :, pl.ds(j * 128, 128)] = qo[j, at, :].astype(BF16)
        o_copy.wait_recv()
        p_copies, own = [], []
        context = jnp.concatenate([ol[:, h].reshape(2 * n_rows, LATENT) for h in range(half)], axis=1)
        for first in range(0, n_d, 2):
            for n in (first, first + 1):
                wo_copy(l, n).wait()
            weights = jnp.concatenate([buf[wo_at(l, n * o_rows, o_rows), :] for n in (first, first + 1)], axis=1)
            acc = dot(context, weights)
            for n in (first, first + 1):
                cols = slice((n - first) * CHUNK, (n - first + 1) * CHUNK)
                own.append(acc[:n_rows, cols])
                for j in range(n_j):
                    outbox[n, pl.ds(j * n_rows, n_rows), :] = acc[n_rows:, cols][:, j * 128:(j + 1) * 128]
                copy = remote(outbox.at[n, pl.ds(0, n_j * n_rows)], pr.at[n], p_sem.at[l, n], peer[1])
                copy.start()
                p_copies.append(copy)
        if l + 1 == n_layers:
            start(head_copy(i) for i in range(HEAD_B))
        for n in range(n_d):
            cols = pl.ds(n * CHUNK, CHUNK)
            p_copies[n].wait_recv()
            theirs = jnp.concatenate([pr[n, pl.ds(j * n_rows, n_rows), :] for j in range(n_j)], axis=1)
            x_cur[:, cols] = (x_cur[:, cols].astype(F32) + (own[n] + theirs)).astype(BF16)

        rows[0] = rms_norm(x_cur[...], gain_ffn[pl.ds(l, 1), :])
        row_sends = gather(rows.at[0], lambda j, k: rows.at[k], ag_sem.at[l])
        if l + 1 < n_layers:
            start(wq_copy(l + 1, n) for n in range(n_q))
        for i in range(2 * n_d):
            ffn_copy(l, i).wait()
        all_rows = rows[...].reshape(NUM_DEV * n_rows, d_model)
        for lo, hi in cuts:
            w_part = [jnp.concatenate([buf[ffn_at(l, (u * n_d + k) * pad_width + lo, hi - lo), :] for k in range(n_d)], axis=1)
                      for u in (0, 1)]
            gate = dot_nt(all_rows, w_part[0])
            up = dot_nt(all_rows, w_part[1])
            act[:, pl.ds(lo, hi - lo)] = (jax.nn.silu(gate) * up).astype(BF16)

        for copy in row_sends + p_copies:
            copy.wait_send()
        pair, chip = [], []

        def reduce_chunk(c):
            pair[c].wait_recv()
            for k in range(4):
                at = pl.ds((c * 4 + k) * n_rows, n_rows)
                for j in range(n_j):
                    lanes = pl.ds(j * 128, 128)
                    both = qo[j, at, :] + pair_in[2 * c + j // 2, pl.ds((j % 2 * 4 + k) * n_rows, n_rows), :]
                    if k == 0:
                        qo[j, at, :] = both
                    else:
                        total[c, k - 1, :, lanes] = both.astype(BF16)
            for k in (3, 1, 2):
                copy = remote(total.at[c, k - 1], chip_in.at[c, k - 1], chip_sem.at[l, c, k - 1], peer[2 * k])
                copy.start()
                chip.append(copy)

        for c in range(n_d):
            ffn_copy(l, 2 * n_d + c).wait()
            y = dot(act[...], buf[ffn_at(l, (2 * n_d + c) * pad_width, width), :])
            y = y.reshape(4, 2, n_rows, CHUNK)
            theirs = y[:, 1].reshape(4 * n_rows, CHUNK)
            for j in range(n_j):
                outbox[2 * c + j // 2, pl.ds(j % 2 * 4 * n_rows, 4 * n_rows), :] = theirs[:, j * 128:(j + 1) * 128]
            mine = y[:, 0].reshape(4 * n_rows, CHUNK)
            for j in range(n_j):
                qo[j, pl.ds(c * 4 * n_rows, 4 * n_rows), :] = mine[:, j * 128:(j + 1) * 128]
            copy = remote(outbox.at[pl.ds(2 * c, 2)], pair_in.at[pl.ds(2 * c, 2)], pair_sem.at[l, c], peer[1])
            copy.start()
            pair.append(copy)
            if c >= 1:
                reduce_chunk(c - 1)
        reduce_chunk(n_d - 1)
        if l + 1 < n_layers:
            start(kv_copy(l + 1, b) for b in range(n_rows))
            start(wo_copy(l + 1, n) for n in range(n_d))
        else:
            start(head_copy(i) for i in range(HEAD_B, HEAD_A))
        for copy in chip:
            copy.wait_recv()
        for c in range(n_d):
            cols = pl.ds(c * CHUNK, CHUNK)
            y = jnp.concatenate([qo[j, pl.ds(c * 4 * n_rows, n_rows), :] for j in range(n_j)], axis=1)
            for k in range(3):
                y = y + chip_in[c, k].astype(F32)
            x_cur[:, cols] = (x_cur[:, cols].astype(F32) + y).astype(BF16)
        for copy in sent + pair + chip:
            copy.wait_send()

    hrows[0] = rms_norm(x_cur[...], gain_fin[...])
    rows[me] = hrows[0]
    peer[0] = me
    sends = gather(hrows.at[0], lambda j, k: rows.at[peer[j]], fin_sem)
    for copy in sends:
        copy.wait_send()
    for i in range(n_vocab):
        head_copy(i).wait()


def head_kernel(dims, rows, buf, out_hbm, tile, sem):
    d_model, vocab = dims
    n_vocab = vocab // CHUNK

    def out_copy(i, cols, slot):
        at = pl.ds(i * 2 * CHUNK if isinstance(i, int) else pl.multiple_of(i * 2 * CHUNK, 128), cols)
        return pltpu.make_async_copy(tile.at[slot, :, pl.ds(0, cols)], out_hbm.at[:, at], sem.at[slot])

    def weights(chunk):
        return buf[pl.ds(pl.multiple_of(head_chunk(chunk) * d_model, 128), d_model), :]

    def step(i, carry):
        slot = lax.rem(i, 2)
        both = dot(rows[...], jnp.concatenate([weights(2 * i), weights(2 * i + 1)], axis=1))

        @pl.when(i >= 2)
        def _():
            out_copy(i - 2, 2 * CHUNK, slot).wait()

        tile[slot] = both
        out_copy(i, 2 * CHUNK, slot).start()
        return carry

    n_pairs = n_vocab // 2
    lax.fori_loop(0, n_pairs, step, 0)
    for i in (n_pairs - 2, n_pairs - 1):
        if i % 2 == n_pairs % 2:
            out_copy(i, 2 * CHUNK, i % 2).wait()
    if n_vocab % 2:
        tile[n_pairs % 2, :, pl.ds(0, CHUNK)] = dot(rows[...], weights(n_vocab - 1))
        out_copy(n_pairs, CHUNK, n_pairs % 2).start()
    out_copy(n_pairs - 1, 2 * CHUNK, (n_pairs - 1) % 2).wait()
    if n_vocab % 2:
        out_copy(n_pairs, CHUNK, n_pairs % 2).wait()


def run_head(rows, buf, vocab):
    n_rows, d_model = rows.shape
    vmem = pl.BlockSpec(memory_space=pltpu.VMEM)
    buf = pltpu.with_memory_space_constraint(buf, pltpu.VMEM)
    return pl.pallas_call(
        functools.partial(head_kernel, (d_model, vocab)),
        out_shape=jax.ShapeDtypeStruct((n_rows, vocab), F32),
        in_specs=[vmem, vmem],
        out_specs=pl.BlockSpec(memory_space=pl.ANY),
        scratch_shapes=[pltpu.VMEM((2, n_rows, 2 * CHUNK), F32), pltpu.SemaphoreType.DMA((2,))],
        compiler_params=pltpu.CompilerParams(vmem_limit_bytes=VMEM_LAYERS),
        name='head',
    )(rows, buf)


def run_layers(hidden, lengths, kv_t, gain_attn, w_q, w_o, gain_ffn, wg_t, wu_t, w_down, gain_fin, w_head):
    n_layers, n_rows, kv_width, seq_len = kv_t.shape
    d_model = hidden.shape[1]
    n_heads = w_q.shape[2] // kv_width
    width = w_down.shape[1]
    pad_width = round_up(width, 16)
    half, n_d = n_heads // 2, d_model // CHUNK
    n_q = half * kv_width // CHUNK
    n_t = round_up(kv_width, 128) // 128
    slot_rows = max(n_q * d_model, n_rows * kv_width, n_d * half * LATENT, 3 * n_d * pad_width)
    dims = (n_layers, n_rows, d_model, n_heads, kv_width, seq_len, width, pad_width, slot_rows, w_head.shape[1])
    vmem, anys = pl.BlockSpec(memory_space=pltpu.VMEM), pl.BlockSpec(memory_space=pl.ANY)
    smem = pl.BlockSpec(memory_space=pltpu.SMEM)
    dma = pltpu.SemaphoreType.DMA
    scratch = [
        pltpu.VMEM((n_rows, d_model), BF16),
        pltpu.VMEM((2, n_rows, d_model), BF16),
        pltpu.VMEM((n_t, n_heads * n_rows, 128), F32),
        pltpu.VMEM((8, half * n_rows, 128), F32),
        pltpu.VMEM((2, GROUP, n_heads, seq_len), BF16),
        pltpu.VMEM((2, half, n_rows, LATENT), BF16),
        pltpu.VMEM((half, n_rows, LATENT), BF16),
        pltpu.VMEM((n_d, CHUNK // 128 * n_rows, 128), F32),
        pltpu.VMEM((NUM_DEV * n_rows, width), BF16),
        pltpu.VMEM((8, half * n_rows, 128), F32),
        pltpu.VMEM((n_d, 3, n_rows, CHUNK), BF16),
        pltpu.VMEM((n_d, 3, n_rows, CHUNK), BF16),
        dma((n_layers, n_q)), dma((n_layers, n_rows)), dma((n_layers, n_d)), dma((n_layers, 3 * n_d)),
        dma((n_layers, 2)), dma((n_layers, half // 2, 2)), dma((n_layers, 2)), dma((n_layers, n_d, 2)),
        dma((n_layers, 8, 2)), dma((n_layers, n_d, 2)), dma((n_layers, n_d, 3, 2)), dma((8, 2)), dma((w_head.shape[1] // CHUNK,)),
    ]
    return pl.pallas_call(
        functools.partial(layers_kernel, dims),
        out_shape=[pltpu.VMEM((NUM_DEV, n_rows, d_model), BF16), pltpu.VMEM((3 * slot_rows, CHUNK), BF16)],
        in_specs=[vmem, smem, vmem, vmem, vmem] + [anys] * 7,
        out_specs=[vmem, vmem],
        scratch_shapes=scratch,
        compiler_params=pltpu.CompilerParams(collective_id=0, has_side_effects=True, vmem_limit_bytes=VMEM_LAYERS),
        name='layers',
    )(hidden, lengths, gain_attn, gain_ffn, gain_fin.reshape(1, -1), kv_t, w_q, w_o, wg_t, wu_t, w_down, w_head)


def solution(mesh):
    row_axes = ('rep', 'dp')
    specs_in = (P(row_axes, None), P(row_axes), P(None, row_axes, None, None), P(), P(), P(), P(),
                P(None, None, 'dp'), P(None, None, 'dp'), P(None, 'dp', None), P(), P(None, 'dp'))

    def device_step(hidden, lengths, kv_cache, norm_attn, w_q, w_o, norm_ffn, w_gate, w_up, w_down, norm_final, w_head):
        rows, buf = run_layers(hidden, lengths, jnp.swapaxes(kv_cache, 2, 3), norm_attn, w_q, w_o, norm_ffn,
                               jnp.swapaxes(w_gate, 1, 2), jnp.swapaxes(w_up, 1, 2), w_down, norm_final, w_head)
        return run_head(rows.reshape(-1, hidden.shape[1]), buf, w_head.shape[1])

    return jax.shard_map(device_step, mesh=mesh, in_specs=specs_in, out_specs=P('rep', 'dp'), check_vma=False)
```

```python
import functools

import jax
import jax.numpy as jnp
from jax import lax
from jax.experimental import pallas as pl
from jax.experimental.pallas import tpu as pltpu
from jax.sharding import PartitionSpec as P

LATENT = 512
QK_SCALE = 192 ** -0.5
NORM_EPS = 1e-6
MESH_ID = pl.DeviceIdType.MESH
NUM_DEV = 8
CHUNK = 512
GROUP = 8
HEAD_A, HEAD_B = 16, 9
VMEM_LAYERS = int(8.9 * 2**20)
BF16, F32 = jnp.bfloat16, jnp.float32


def rms_norm(x_rows, gain_vec):
    x_float = x_rows.astype(F32)
    inv_rms = lax.rsqrt(jnp.mean(x_float * x_float, axis=-1, keepdims=True) + NORM_EPS)
    return (x_float * inv_rms * gain_vec).astype(BF16)


def dot(a, b):
    return jnp.dot(a, b, preferred_element_type=F32)


def dot_nt(a, b):
    return lax.dot_general(a, b, (((1,), (1,)), ((), ())), preferred_element_type=F32)


def round_up(n, m):
    return (n + m - 1) // m * m


def head_chunk(i):
    return i + i // HEAD_A * 2


def cuts_of(width):
    return [(lo, min(lo + CHUNK, width)) for lo in range(0, width, CHUNK)]


def layers_kernel(dims, x_ref, len_ref, gain_attn, gain_ffn, gain_fin, kv_hbm, wq_hbm, wo_hbm, wg_hbm, wu_hbm, wd_hbm,
                  wh_hbm, rows, buf, x_cur, hrows, qo, outbox, p_buf, ol, ol_send, pr, act, pair_in, total, chip_in,
                  wq_sem, kv_sem, wo_sem, ffn_sem, h_sem, q_sem, o_sem, p_sem, ag_sem, pair_sem, chip_sem, fin_sem, head_sem):
    n_layers, n_rows, d_model, n_heads, kv_width, seq_len, width, pad_width, slot_rows, vocab = dims
    half = n_heads // 2
    q_cols = half * kv_width
    n_q, n_d = q_cols // CHUNK, d_model // CHUNK
    o_rows = half * LATENT
    n_t, n_j = round_up(kv_width, 128) // 128, CHUNK // 128
    cuts = cuts_of(width)
    n_vocab = vocab // CHUNK

    me = lax.axis_index('dp')
    core, x_pos, y_pos = me % 2, (me // 2) % 2, me // 4
    flip = lambda c, a, b: ((y_pos + b) % 2) * 4 + ((x_pos + a) % 2) * 2 + (core + c) % 2
    peer = {1: flip(1, 0, 0), 2: flip(0, 1, 0), 4: flip(0, 0, 1), 6: flip(0, 1, 1)}
    other = 1 - core

    def remote(src, dst, sems, dev):
        return pltpu.make_async_remote_copy(src_ref=src, dst_ref=dst, send_sem=sems.at[0], recv_sem=sems.at[1],
                                            device_id={'dp': dev}, device_id_type=MESH_ID)

    wq_at = lambda l, row, n: pl.ds(l % 3 * slot_rows + row, n)
    kv_at = lambda l, row, n: pl.ds((l + 1) % 3 * slot_rows + row, n)
    wo_at = lambda l, row, n: pl.ds((l + 2) % 3 * slot_rows + row, n)
    ffn_at = wq_at

    def wq_copy(l, n):
        cols = pl.ds(pl.multiple_of(core * q_cols + n * CHUNK, 128), CHUNK)
        return pltpu.make_async_copy(wq_hbm.at[l, :, cols], buf.at[wq_at(l, n * d_model, d_model)], wq_sem.at[l, n])

    def kv_copy(l, b):
        row = b * kv_width if isinstance(b, int) else pl.multiple_of(b * kv_width, 64)
        return pltpu.make_async_copy(kv_hbm.at[l, b], buf.at[kv_at(l, row, kv_width)], kv_sem.at[l, b])

    def wo_copy(l, n):
        src = wo_hbm.at[l, pl.ds(pl.multiple_of(core * o_rows, 128), o_rows), pl.ds(n * CHUNK, CHUNK)]
        return pltpu.make_async_copy(src, buf.at[wo_at(l, n * o_rows, o_rows)], wo_sem.at[l, n])

    def ffn_copy(l, i):
        src = (wg_hbm, wu_hbm, wd_hbm)[i // n_d]
        return pltpu.make_async_copy(src.at[l, :, pl.ds((i % n_d) * CHUNK, CHUNK)],
                                     buf.at[ffn_at(l, i * pad_width, width)], ffn_sem.at[l, i])

    def head_copy(i):
        row = head_chunk(i) * d_model
        return pltpu.make_async_copy(wh_hbm.at[:, pl.ds(i * CHUNK, CHUNK)], buf.at[pl.ds(row, d_model)], head_sem.at[i])

    def start(copies):
        for copy in copies:
            copy.start()

    def gather(own, block, sems):
        every, size = [], n_rows // 4
        chunk = lambda ref, c: ref.at[pl.ds(c * size, size)]

        def send(src, j, k):
            copy = remote(src, block(j, k), sems.at[len(every)], peer[k])
            copy.start()
            every.append(copy)
            return copy

        def send_chunk(src, c, j, k):
            copy = remote(chunk(src, c), chunk(block(j, k), c), sems.at[len(every)], peer[k])
            copy.start()
            every.append(copy)
            return copy

        x_order, y_order = (0, 1, 2, 3), (2, 3, 0, 1)
        near = {}
        for cx, cy in zip(x_order, y_order):
            near[2, cx] = send_chunk(own, cx, 0, 2)
            near[4, cy] = send_chunk(own, cy, 0, 4)
        arrivals = [send(own, 0, 1)]
        far = {}
        for i in range(4):
            for j, c in ((2, x_order[i]), (4, y_order[i])):
                near[j, c].wait_recv()
                if i < 2:
                    far[c] = send_chunk(block(j, 0), c, j, 6 - j)
                arrivals.append(send_chunk(block(j, 0), c, j, 1))
        for c in (0, 2, 1, 3):
            far[c].wait_recv()
            arrivals.append(send_chunk(block(6, 0), c, 6, 1))
        for copy in arrivals:
            copy.wait_recv()
        return every

    start(wq_copy(0, n) for n in range(n_q))
    x_cur[...] = x_ref[...]

    for l in range(n_layers):
        sent = []
        hrows[0] = rms_norm(x_cur[...], gain_attn[pl.ds(l, 1), :])
        if l == 0:
            barrier = pltpu.get_barrier_semaphore()
            for j in (1, 2, 4, 6):
                pl.semaphore_signal(barrier, inc=1, device_id={'dp': peer[j]}, device_id_type=MESH_ID)
            pl.semaphore_wait(barrier, 4)
        copy = remote(hrows.at[0], hrows.at[1], h_sem.at[l], peer[1])
        copy.start()
        sent.append(copy)
        copy.wait_recv()
        both_rows = hrows[...].reshape(2 * n_rows, d_model)
        prev, q_copies = None, []
        for first in range(0, n_q, 3):
            for n in range(first, first + 3):
                wq_copy(l, n).wait()
            if l == 0:
                per = -(-3 * n_rows // n_q)
                start(kv_copy(l, b) for b in range(first // 3 * per, min((first // 3 + 1) * per, n_rows)))
            weights = jnp.concatenate([buf[wq_at(l, n * d_model, d_model), :] for n in range(first, first + 3)], axis=1)
            wide = dot(both_rows, weights).astype(BF16).astype(F32)
            for n in range(first, first + 3):
                cur = wide[:, (n - first) * CHUNK:(n - first + 1) * CHUNK]
                if n >= 1:
                    h = n - 1
                    off = h * kv_width - h * CHUNK
                    q_head = jnp.concatenate([prev[:, off:], cur[:, :off + kv_width - CHUNK]], axis=1)
                    for j in range(n_t):
                        lanes = slice(j * 128, min((j + 1) * 128, kv_width))
                        keep = pl.ds(0, lanes.stop - lanes.start)
                        at = pl.ds(pl.multiple_of((core * half + h) * n_rows, n_rows), n_rows)
                        qo[j, at, keep] = q_head[:n_rows, lanes]
                        outbox[j, pl.ds(h * n_rows, n_rows), keep] = q_head[n_rows:, lanes]
                    if h % 2:
                        dst = qo.at[:, pl.ds(pl.multiple_of((core * half + h - 1) * n_rows, n_rows), 2 * n_rows)]
                        copy = remote(outbox.at[pl.ds(0, n_t), pl.ds((h - 1) * n_rows, 2 * n_rows)], dst, q_sem.at[l, h // 2], peer[1])
                        copy.start()
                        q_copies.append(copy)
                prev = cur
        if l == 0:
            start(wo_copy(l, n) for n in range(n_d))
        for copy in q_copies:
            copy.wait_recv()

        key_pos = lax.broadcasted_iota(jnp.int32, (n_heads, seq_len), 1)

        def scores(g, l=l):
            slot = lax.rem(g, 2)
            for i in range(GROUP):
                kv_copy(l, g * GROUP + i).wait()
            for i in range(GROUP):
                b = g * GROUP + i
                q = [qo[j, pl.ds(b, n_heads, stride=n_rows), :].astype(BF16) for j in range(n_t)]
                q = jnp.concatenate(q, axis=1)[:, :kv_width]
                row = pl.multiple_of(b * kv_width, 64)
                s = dot(q, buf[kv_at(l, row, kv_width), :]) * QK_SCALE
                s = jnp.where(key_pos < len_ref[b], s, -1e30)
                e = jnp.exp(s - jnp.max(s, axis=-1, keepdims=True))
                p_buf[slot, i] = (e / jnp.sum(e, axis=-1, keepdims=True)).astype(BF16)

        def contexts(g, l=l):
            slot = lax.rem(g, 2)
            for i in range(GROUP):
                b = g * GROUP + i
                row = pl.multiple_of(b * kv_width, 64)
                ctx = dot_nt(p_buf[slot, i], buf[kv_at(l, row, LATENT), :])
                for j in range(n_j):
                    qo[j, pl.ds(b, n_heads, stride=n_rows), :] = ctx[:, j * 128:(j + 1) * 128]

        n_groups = n_rows // GROUP
        scores(jnp.int32(0))

        def step(g, carry):
            scores(g)
            contexts(g - 1)
            return carry

        lax.fori_loop(1, n_groups, step, 0)
        contexts(jnp.int32(n_groups - 1))
        if l + 1 == n_layers:
            start(head_copy(i) for i in range(HEAD_A, n_vocab))

        for copy in q_copies:
            copy.wait_send()

        for h in range(half):
            at = pl.ds(pl.multiple_of((other * half + h) * n_rows, n_rows), n_rows)
            for j in range(n_j):
                ol_send[h, :, pl.ds(j * 128, 128)] = qo[j, at, :].astype(BF16)
        o_copy = remote(ol_send, ol.at[1], o_sem.at[l], peer[1])
        o_copy.start()
        sent.append(o_copy)
        start(ffn_copy(l, i) for i in range(3 * n_d))
        for h in range(half):
            at = pl.ds(pl.multiple_of((core * half + h) * n_rows, n_rows), n_rows)
            for j in range(n_j):
                ol[0, h, :, pl.ds(j * 128, 128)] = qo[j, at, :].astype(BF16)
        o_copy.wait_recv()
        p_copies, own = [], []
        context = jnp.concatenate([ol[:, h].reshape(2 * n_rows, LATENT) for h in range(half)], axis=1)
        for first in range(0, n_d, 2):
            for n in (first, first + 1):
                wo_copy(l, n).wait()
            weights = jnp.concatenate([buf[wo_at(l, n * o_rows, o_rows), :] for n in (first, first + 1)], axis=1)
            acc = dot(context, weights)
            for n in (first, first + 1):
                cols = slice((n - first) * CHUNK, (n - first + 1) * CHUNK)
                own.append(acc[:n_rows, cols])
                for j in range(n_j):
                    outbox[n, pl.ds(j * n_rows, n_rows), :] = acc[n_rows:, cols][:, j * 128:(j + 1) * 128]
                copy = remote(outbox.at[n, pl.ds(0, n_j * n_rows)], pr.at[n], p_sem.at[l, n], peer[1])
                copy.start()
                p_copies.append(copy)
        if l + 1 == n_layers:
            start(head_copy(i) for i in range(HEAD_B))
        for n in range(n_d):
            cols = pl.ds(n * CHUNK, CHUNK)
            p_copies[n].wait_recv()
            theirs = jnp.concatenate([pr[n, pl.ds(j * n_rows, n_rows), :] for j in range(n_j)], axis=1)
            x_cur[:, cols] = (x_cur[:, cols].astype(F32) + (own[n] + theirs)).astype(BF16)

        rows[0] = rms_norm(x_cur[...], gain_ffn[pl.ds(l, 1), :])
        row_sends = gather(rows.at[0], lambda j, k: rows.at[j ^ k], ag_sem.at[l])
        if l + 1 < n_layers:
            start(wq_copy(l + 1, n) for n in range(n_q))
        for i in range(2 * n_d):
            ffn_copy(l, i).wait()
        all_rows = rows[...].reshape(NUM_DEV * n_rows, d_model)
        for lo, hi in cuts:
            w_part = [jnp.concatenate([buf[ffn_at(l, (u * n_d + k) * pad_width + lo, hi - lo), :] for k in range(n_d)], axis=1)
                      for u in (0, 1)]
            gate = dot_nt(all_rows, w_part[0])
            up = dot_nt(all_rows, w_part[1])
            act[:, pl.ds(lo, hi - lo)] = (jax.nn.silu(gate) * up).astype(BF16)

        for copy in row_sends + p_copies:
            copy.wait_send()
        pair, chip, relay = [], [], []
        first, second = (1, 2, 1, 2), (2, 1, 2, 1)

        def reduce_chunk(c):
            pair[c].wait_recv()
            for k in range(4):
                at = pl.ds((c * 4 + k) * n_rows, n_rows)
                for j in range(n_j):
                    lanes = pl.ds(j * 128, 128)
                    both = qo[j, at, :] + pair_in[2 * c + j // 2, pl.ds((j % 2 * 4 + k) * n_rows, n_rows), :]
                    if k in (0, second[c]):
                        qo[j, at, :] = both
                    else:
                        total[c, k // 3, :, lanes] = both.astype(BF16)
            for i in (1, 0):
                copy = remote(total.at[c, i], chip_in.at[c, i], chip_sem.at[l, c, i], peer[2 * first[c]])
                copy.start()
                chip.append(copy)

        def relay_chunk(c):
            chip[2 * c].wait_recv()
            at = pl.ds((c * 4 + second[c]) * n_rows, n_rows)
            for j in range(n_j):
                lanes = pl.ds(j * 128, 128)
                total[c, 2, :, lanes] = (qo[j, at, :] + chip_in[c, 1, :, lanes].astype(F32)).astype(BF16)
            copy = remote(total.at[c, 2], chip_in.at[c, 2], chip_sem.at[l, c, 2], peer[2 * second[c]])
            copy.start()
            relay.append(copy)

        for c in range(n_d):
            ffn_copy(l, 2 * n_d + c).wait()
            y = dot(act[...], buf[ffn_at(l, (2 * n_d + c) * pad_width, width), :])
            y = y.reshape(4, 2, n_rows, CHUNK)
            theirs = y[:, 1].reshape(4 * n_rows, CHUNK)
            for j in range(n_j):
                outbox[2 * c + j // 2, pl.ds(j % 2 * 4 * n_rows, 4 * n_rows), :] = theirs[:, j * 128:(j + 1) * 128]
            mine = y[:, 0].reshape(4 * n_rows, CHUNK)
            for j in range(n_j):
                qo[j, pl.ds(c * 4 * n_rows, 4 * n_rows), :] = mine[:, j * 128:(j + 1) * 128]
            copy = remote(outbox.at[pl.ds(2 * c, 2)], pair_in.at[pl.ds(2 * c, 2)], pair_sem.at[l, c], peer[1])
            copy.start()
            pair.append(copy)
            if c >= 1:
                reduce_chunk(c - 1)
        reduce_chunk(n_d - 1)
        for c in range(n_d):
            relay_chunk(c)
        if l + 1 < n_layers:
            start(kv_copy(l + 1, b) for b in range(n_rows))
            start(wo_copy(l + 1, n) for n in range(n_d))
        else:
            start(head_copy(i) for i in range(HEAD_B, HEAD_A))
        for copy in chip[1::2] + relay:
            copy.wait_recv()
        for c in range(n_d):
            cols = pl.ds(c * CHUNK, CHUNK)
            y = jnp.concatenate([qo[j, pl.ds(c * 4 * n_rows, n_rows), :] for j in range(n_j)], axis=1)
            for i in (0, 2):
                y = y + chip_in[c, i].astype(F32)
            x_cur[:, cols] = (x_cur[:, cols].astype(F32) + y).astype(BF16)
        for copy in sent + pair + chip + relay:
            copy.wait_send()

    hrows[0] = rms_norm(x_cur[...], gain_fin[...])
    rows[me] = hrows[0]
    peer[0] = me
    sends = gather(hrows.at[0], lambda j, k: rows.at[peer[j]], fin_sem)
    for copy in sends:
        copy.wait_send()
    for i in range(n_vocab):
        head_copy(i).wait()


def head_kernel(dims, rows, buf, out_hbm, tile, sem):
    d_model, vocab = dims
    n_vocab = vocab // CHUNK

    def out_copy(i, cols, slot):
        at = pl.ds(i * 2 * CHUNK if isinstance(i, int) else pl.multiple_of(i * 2 * CHUNK, 128), cols)
        return pltpu.make_async_copy(tile.at[slot, :, pl.ds(0, cols)], out_hbm.at[:, at], sem.at[slot])

    def weights(chunk):
        return buf[pl.ds(pl.multiple_of(head_chunk(chunk) * d_model, 128), d_model), :]

    def step(i, carry):
        half = lax.rem(i, 2) * 2

        @pl.when(i >= 2)
        def _():
            for h in (0, 1):
                out_copy(2 * i - 4 + h, 2 * CHUNK, half + h).wait()

        for c in range(4):
            tile[half + c // 2, :, pl.ds(c % 2 * CHUNK, CHUNK)] = dot(x, weights(4 * i + c))
        for h in (0, 1):
            out_copy(2 * i + h, 2 * CHUNK, half + h).start()
        return carry

    x = rows[...].reshape(-1, d_model)
    n_quads = n_vocab // 4
    lax.fori_loop(0, n_quads, step, 0)
    for i in range(max(n_quads - 2, 0), n_quads):
        for h in (0, 1):
            out_copy(2 * i + h, 2 * CHUNK, i % 2 * 2 + h).wait()
        if i == n_quads - 2 and n_vocab % 4:
            last = n_quads % 2 * 2
            tile[last, :, pl.ds(0, CHUNK)] = dot(x, weights(n_vocab - 1))
            out_copy(2 * n_quads, CHUNK, last).start()
    if n_vocab % 4:
        out_copy(2 * n_quads, CHUNK, n_quads % 2 * 2).wait()


def run_head(rows, buf, vocab):
    n_rows, d_model = rows.shape[0] * rows.shape[1], rows.shape[2]
    vmem = pl.BlockSpec(memory_space=pltpu.VMEM)
    rows, buf = (pltpu.with_memory_space_constraint(a, pltpu.VMEM) for a in (rows, buf))
    return pl.pallas_call(
        functools.partial(head_kernel, (d_model, vocab)),
        out_shape=jax.ShapeDtypeStruct((n_rows, vocab), F32),
        in_specs=[vmem, vmem],
        out_specs=pl.BlockSpec(memory_space=pl.ANY),
        scratch_shapes=[pltpu.VMEM((4, n_rows, 2 * CHUNK), F32), pltpu.SemaphoreType.DMA((4,))],
        compiler_params=pltpu.CompilerParams(vmem_limit_bytes=VMEM_LAYERS),
        name='head',
    )(rows, buf)


def run_layers(hidden, lengths, kv_t, gain_attn, w_q, w_o, gain_ffn, wg_t, wu_t, w_down, gain_fin, w_head):
    n_layers, n_rows, kv_width, seq_len = kv_t.shape
    d_model = hidden.shape[1]
    n_heads = w_q.shape[2] // kv_width
    width = w_down.shape[1]
    pad_width = round_up(width, 16)
    half, n_d = n_heads // 2, d_model // CHUNK
    n_q = half * kv_width // CHUNK
    n_t = round_up(kv_width, 128) // 128
    slot_rows = max(n_q * d_model, n_rows * kv_width, n_d * half * LATENT, 3 * n_d * pad_width)
    dims = (n_layers, n_rows, d_model, n_heads, kv_width, seq_len, width, pad_width, slot_rows, w_head.shape[1])
    vmem, anys = pl.BlockSpec(memory_space=pltpu.VMEM), pl.BlockSpec(memory_space=pl.ANY)
    smem = pl.BlockSpec(memory_space=pltpu.SMEM)
    dma = pltpu.SemaphoreType.DMA
    scratch = [
        pltpu.VMEM((n_rows, d_model), BF16),
        pltpu.VMEM((2, n_rows, d_model), BF16),
        pltpu.VMEM((n_t, n_heads * n_rows, 128), F32),
        pltpu.VMEM((8, half * n_rows, 128), F32),
        pltpu.VMEM((2, GROUP, n_heads, seq_len), BF16),
        pltpu.VMEM((2, half, n_rows, LATENT), BF16),
        pltpu.VMEM((half, n_rows, LATENT), BF16),
        pltpu.VMEM((n_d, CHUNK // 128 * n_rows, 128), F32),
        pltpu.VMEM((NUM_DEV * n_rows, width), BF16),
        pltpu.VMEM((8, half * n_rows, 128), F32),
        pltpu.VMEM((n_d, 3, n_rows, CHUNK), BF16),
        pltpu.VMEM((n_d, 3, n_rows, CHUNK), BF16),
        dma((n_layers, n_q)), dma((n_layers, n_rows)), dma((n_layers, n_d)), dma((n_layers, 3 * n_d)),
        dma((n_layers, 2)), dma((n_layers, half // 2, 2)), dma((n_layers, 2)), dma((n_layers, n_d, 2)),
        dma((n_layers, 25, 2)), dma((n_layers, n_d, 2)), dma((n_layers, n_d, 3, 2)), dma((25, 2)), dma((w_head.shape[1] // CHUNK,)),
    ]
    return pl.pallas_call(
        functools.partial(layers_kernel, dims),
        out_shape=[pltpu.VMEM((NUM_DEV, n_rows, d_model), BF16), pltpu.VMEM((3 * slot_rows, CHUNK), BF16)],
        in_specs=[vmem, smem, vmem, vmem, vmem] + [anys] * 7,
        out_specs=[vmem, vmem],
        scratch_shapes=scratch,
        compiler_params=pltpu.CompilerParams(collective_id=0, has_side_effects=True, vmem_limit_bytes=VMEM_LAYERS),
        name='layers',
    )(hidden, lengths, gain_attn, gain_ffn, gain_fin.reshape(1, -1), kv_t, w_q, w_o, wg_t, wu_t, w_down, w_head)


def solution(mesh):
    row_axes = ('rep', 'dp')
    specs_in = (P(row_axes, None), P(row_axes), P(None, row_axes, None, None), P(), P(), P(), P(),
                P(None, None, 'dp'), P(None, None, 'dp'), P(None, 'dp', None), P(), P(None, 'dp'))

    def device_step(hidden, lengths, kv_cache, norm_attn, w_q, w_o, norm_ffn, w_gate, w_up, w_down, norm_final, w_head):
        rows, buf = run_layers(hidden, lengths, jnp.swapaxes(kv_cache, 2, 3), norm_attn, w_q, w_o, norm_ffn,
                               jnp.swapaxes(w_gate, 1, 2), jnp.swapaxes(w_up, 1, 2), w_down, norm_final, w_head)
        return run_head(rows, buf, w_head.shape[1])

    return jax.shard_map(device_step, mesh=mesh, in_specs=specs_in, out_specs=P('rep', 'dp'), check_vma=False)
```

```python
import functools

import jax
import jax.numpy as jnp
from jax import lax
from jax.experimental import pallas as pl
from jax.experimental.pallas import tpu as pltpu
from jax.sharding import PartitionSpec as P

LATENT = 512
QK_SCALE = 192 ** -0.5
NORM_EPS = 1e-6
MESH_ID = pl.DeviceIdType.MESH
NUM_DEV = 8
CHUNK, RS_CHUNK = 512, 256
GROUP = 8
HEAD_A, HEAD_B = 16, 9
VMEM_LAYERS = int(8.9 * 2**20)
BF16, F32 = jnp.bfloat16, jnp.float32


def rms_norm(x_rows, gain_vec):
    x_float = x_rows.astype(F32)
    inv_rms = lax.rsqrt(jnp.mean(x_float * x_float, axis=-1, keepdims=True) + NORM_EPS)
    return (x_float * inv_rms * gain_vec).astype(BF16)


def dot(a, b):
    return jnp.dot(a, b, preferred_element_type=F32)


def dot_nt(a, b):
    return lax.dot_general(a, b, (((1,), (1,)), ((), ())), preferred_element_type=F32)


def round_up(n, m):
    return (n + m - 1) // m * m


def head_chunk(i):
    return i + i // HEAD_A * 2


def cuts_of(width):
    return [(lo, min(lo + CHUNK, width)) for lo in range(0, width, CHUNK)]


def layers_kernel(dims, x_ref, len_ref, gain_attn, gain_ffn, gain_fin, kv_hbm, wq_hbm, wo_hbm, wg_hbm, wu_hbm, wd_hbm,
                  wh_hbm, rows, buf, x_cur, hrows, qo, outbox, p_buf, ol, ol_send, pr, act, pair_in, total, chip_in,
                  wq_sem, kv_sem, wo_sem, ffn_sem, h_sem, q_sem, o_sem, p_sem, ag_sem, pair_sem, chip_sem, fin_sem, head_sem):
    n_layers, n_rows, d_model, n_heads, kv_width, seq_len, width, pad_width, slot_rows, vocab = dims
    half = n_heads // 2
    q_cols = half * kv_width
    n_q, n_d = q_cols // CHUNK, d_model // CHUNK
    o_rows = half * LATENT
    n_t, n_j = round_up(kv_width, 128) // 128, CHUNK // 128
    cuts = cuts_of(width)
    n_vocab = vocab // CHUNK

    me = lax.axis_index('dp')
    core, x_pos, y_pos = me % 2, (me // 2) % 2, me // 4
    flip = lambda c, a, b: ((y_pos + b) % 2) * 4 + ((x_pos + a) % 2) * 2 + (core + c) % 2
    peer = {1: flip(1, 0, 0), 2: flip(0, 1, 0), 4: flip(0, 0, 1), 6: flip(0, 1, 1)}
    other = 1 - core

    def remote(src, dst, sems, dev):
        return pltpu.make_async_remote_copy(src_ref=src, dst_ref=dst, send_sem=sems.at[0], recv_sem=sems.at[1],
                                            device_id={'dp': dev}, device_id_type=MESH_ID)

    wq_at = lambda l, row, n: pl.ds(l % 3 * slot_rows + row, n)
    kv_at = lambda l, row, n: pl.ds((l + 1) % 3 * slot_rows + row, n)
    wo_at = lambda l, row, n: pl.ds((l + 2) % 3 * slot_rows + row, n)
    ffn_at = wq_at

    def wq_copy(l, n):
        cols = pl.ds(pl.multiple_of(core * q_cols + n * CHUNK, 128), CHUNK)
        return pltpu.make_async_copy(wq_hbm.at[l, :, cols], buf.at[wq_at(l, n * d_model, d_model)], wq_sem.at[l, n])

    def kv_copy(l, b):
        row = b * kv_width if isinstance(b, int) else pl.multiple_of(b * kv_width, 64)
        return pltpu.make_async_copy(kv_hbm.at[l, b], buf.at[kv_at(l, row, kv_width)], kv_sem.at[l, b])

    def wo_copy(l, n):
        src = wo_hbm.at[l, pl.ds(pl.multiple_of(core * o_rows, 128), o_rows), pl.ds(n * CHUNK, CHUNK)]
        return pltpu.make_async_copy(src, buf.at[wo_at(l, n * o_rows, o_rows)], wo_sem.at[l, n])

    def ffn_copy(l, i):
        src = (wg_hbm, wu_hbm, wd_hbm)[i // n_d]
        return pltpu.make_async_copy(src.at[l, :, pl.ds((i % n_d) * CHUNK, CHUNK)],
                                     buf.at[ffn_at(l, i * pad_width, width)], ffn_sem.at[l, i])

    def head_copy(i):
        row = head_chunk(i) * d_model
        return pltpu.make_async_copy(wh_hbm.at[:, pl.ds(i * CHUNK, CHUNK)], buf.at[pl.ds(row, d_model)], head_sem.at[i])

    def start(copies):
        for copy in copies:
            copy.start()

    def gather(own, block, sems):
        every, size = [], n_rows // 4
        chunk = lambda ref, c: ref.at[pl.ds(c * size, size)]

        def send(src, j, k):
            copy = remote(src, block(j, k), sems.at[len(every)], peer[k])
            copy.start()
            every.append(copy)
            return copy

        def send_chunk(src, c, j, k):
            copy = remote(chunk(src, c), chunk(block(j, k), c), sems.at[len(every)], peer[k])
            copy.start()
            every.append(copy)
            return copy

        x_order, y_order = (0, 1, 2, 3), (2, 3, 0, 1)
        near = {}
        for cx, cy in zip(x_order, y_order):
            near[2, cx] = send_chunk(own, cx, 0, 2)
            near[4, cy] = send_chunk(own, cy, 0, 4)
        arrivals = [send(own, 0, 1)]
        far = {}
        for i in range(4):
            for j, c in ((2, x_order[i]), (4, y_order[i])):
                near[j, c].wait_recv()
                if i < 2:
                    far[c] = send_chunk(block(j, 0), c, j, 6 - j)
                arrivals.append(send_chunk(block(j, 0), c, j, 1))
        for c in (0, 2, 1, 3):
            far[c].wait_recv()
            arrivals.append(send_chunk(block(6, 0), c, 6, 1))
        for copy in arrivals:
            copy.wait_recv()
        return every

    start(wq_copy(0, n) for n in range(n_q))
    x_cur[...] = x_ref[...]

    for l in range(n_layers):
        sent = []
        hrows[0] = rms_norm(x_cur[...], gain_attn[pl.ds(l, 1), :])
        if l == 0:
            barrier = pltpu.get_barrier_semaphore()
            for j in (1, 2, 4, 6):
                pl.semaphore_signal(barrier, inc=1, device_id={'dp': peer[j]}, device_id_type=MESH_ID)
            pl.semaphore_wait(barrier, 4)
        copy = remote(hrows.at[0], hrows.at[1], h_sem.at[l], peer[1])
        copy.start()
        sent.append(copy)
        copy.wait_recv()
        both_rows = hrows[...].reshape(2 * n_rows, d_model)
        prev, q_copies = None, []
        bounds = [(i, min(i + 3, n_q)) for i in range(0, n_q, 3)]
        if l == 0:
            bounds[-1:] = [(n_q - 3, n_q - 1), (n_q - 1, n_q)]
        for first, stop in bounds:
            for n in range(first, stop):
                wq_copy(l, n).wait()
            if l == 0:
                start(kv_copy(l, b) for b in range(first * n_rows // n_q, stop * n_rows // n_q))
            weights = jnp.concatenate([buf[wq_at(l, n * d_model, d_model), :] for n in range(first, stop)], axis=1)
            wide = dot(both_rows, weights).astype(BF16).astype(F32)
            for n in range(first, stop):
                cur = wide[:, (n - first) * CHUNK:(n - first + 1) * CHUNK]
                if n >= 1:
                    h = n - 1
                    off = h * kv_width - h * CHUNK
                    q_head = jnp.concatenate([prev[:, off:], cur[:, :off + kv_width - CHUNK]], axis=1)
                    for j in range(n_t):
                        lanes = slice(j * 128, min((j + 1) * 128, kv_width))
                        keep = pl.ds(0, lanes.stop - lanes.start)
                        at = pl.ds(pl.multiple_of((core * half + h) * n_rows, n_rows), n_rows)
                        qo[j, at, keep] = q_head[:n_rows, lanes]
                        outbox[j, pl.ds(h * n_rows, n_rows), keep] = q_head[n_rows:, lanes]
                    if h % 2:
                        dst = qo.at[:, pl.ds(pl.multiple_of((core * half + h - 1) * n_rows, n_rows), 2 * n_rows)]
                        copy = remote(outbox.at[pl.ds(0, n_t), pl.ds((h - 1) * n_rows, 2 * n_rows)], dst, q_sem.at[l, h // 2], peer[1])
                        copy.start()
                        q_copies.append(copy)
                prev = cur
        if l == 0:
            start(wo_copy(l, n) for n in range(n_d))
        for copy in q_copies:
            copy.wait_recv()

        key_pos = lax.broadcasted_iota(jnp.int32, (n_heads, seq_len), 1)

        def scores(g, l=l):
            slot = lax.rem(g, 2)
            for i in range(GROUP):
                kv_copy(l, g * GROUP + i).wait()
            for i in range(GROUP):
                b = g * GROUP + i
                q = [qo[j, pl.ds(b, n_heads, stride=n_rows), :].astype(BF16) for j in range(n_t)]
                q = jnp.concatenate(q, axis=1)[:, :kv_width]
                row = pl.multiple_of(b * kv_width, 64)
                s = dot(q, buf[kv_at(l, row, kv_width), :]) * QK_SCALE
                s = jnp.where(key_pos < len_ref[b], s, -1e30)
                e = jnp.exp(s - jnp.max(s, axis=-1, keepdims=True))
                p_buf[slot, i] = (e / jnp.sum(e, axis=-1, keepdims=True)).astype(BF16)

        def contexts(g, l=l):
            slot = lax.rem(g, 2)
            for i in range(GROUP):
                b = g * GROUP + i
                row = pl.multiple_of(b * kv_width, 64)
                ctx = dot_nt(p_buf[slot, i], buf[kv_at(l, row, LATENT), :])
                for j in range(n_j):
                    qo[j, pl.ds(b, n_heads, stride=n_rows), :] = ctx[:, j * 128:(j + 1) * 128]

        n_groups = n_rows // GROUP
        scores(jnp.int32(0))

        def step(g, carry):
            scores(g)
            contexts(g - 1)
            return carry

        lax.fori_loop(1, n_groups, step, 0)
        contexts(jnp.int32(n_groups - 1))
        if l + 1 == n_layers:
            start(head_copy(i) for i in range(HEAD_A, n_vocab))

        for copy in q_copies:
            copy.wait_send()

        for h in range(half):
            at = pl.ds(pl.multiple_of((other * half + h) * n_rows, n_rows), n_rows)
            for j in range(n_j):
                ol_send[h, :, pl.ds(j * 128, 128)] = qo[j, at, :].astype(BF16)
        o_copy = remote(ol_send, ol.at[1], o_sem.at[l], peer[1])
        o_copy.start()
        sent.append(o_copy)
        start(ffn_copy(l, i) for i in range(3 * n_d))
        for h in range(half):
            at = pl.ds(pl.multiple_of((core * half + h) * n_rows, n_rows), n_rows)
            for j in range(n_j):
                ol[0, h, :, pl.ds(j * 128, 128)] = qo[j, at, :].astype(BF16)
        o_copy.wait_recv()
        p_copies, own = [], []
        context = jnp.concatenate([ol[:, h].reshape(2 * n_rows, LATENT) for h in range(half)], axis=1)
        for first in range(0, n_d, 2):
            for n in (first, first + 1):
                wo_copy(l, n).wait()
            weights = jnp.concatenate([buf[wo_at(l, n * o_rows, o_rows), :] for n in (first, first + 1)], axis=1)
            acc = dot(context, weights)
            for n in (first, first + 1):
                cols = slice((n - first) * CHUNK, (n - first + 1) * CHUNK)
                own.append(acc[:n_rows, cols])
                for j in range(n_j):
                    outbox[n, pl.ds(j * n_rows, n_rows), :] = acc[n_rows:, cols][:, j * 128:(j + 1) * 128]
                copy = remote(outbox.at[n, pl.ds(0, n_j * n_rows)], pr.at[n], p_sem.at[l, n], peer[1])
                copy.start()
                p_copies.append(copy)
        if l + 1 == n_layers:
            start(head_copy(i) for i in range(HEAD_B))
        for n in range(n_d):
            cols = pl.ds(n * CHUNK, CHUNK)
            p_copies[n].wait_recv()
            theirs = jnp.concatenate([pr[n, pl.ds(j * n_rows, n_rows), :] for j in range(n_j)], axis=1)
            x_cur[:, cols] = (x_cur[:, cols].astype(F32) + (own[n] + theirs)).astype(BF16)

        rows[0] = rms_norm(x_cur[...], gain_ffn[pl.ds(l, 1), :])
        row_sends = gather(rows.at[0], lambda j, k: rows.at[j ^ k], ag_sem.at[l])
        if l + 1 < n_layers:
            start(wq_copy(l + 1, n) for n in range(n_q))
        for i in range(2 * n_d):
            ffn_copy(l, i).wait()
        all_rows = rows[...].reshape(NUM_DEV * n_rows, d_model)
        for lo, hi in cuts:
            w_part = [jnp.concatenate([buf[ffn_at(l, (u * n_d + k) * pad_width + lo, hi - lo), :] for k in range(n_d)], axis=1)
                      for u in (0, 1)]
            gate = dot_nt(all_rows, w_part[0])
            up = dot_nt(all_rows, w_part[1])
            act[:, pl.ds(lo, hi - lo)] = (jax.nn.silu(gate) * up).astype(BF16)

        for copy in row_sends + p_copies:
            copy.wait_send()
        pair, chip, relay = [], [], []
        n_r, n_i = d_model // RS_CHUNK, RS_CHUNK // 128
        first = [1 + c % 2 for c in range(n_r)]
        second = [3 - k for k in first]
        kept = lambda c, i, k, n: (n_i * (c // 4) + i, pl.ds((c % 4 * 4 + k) * n_rows, n * n_rows))

        def reduce_chunk(c):
            pair[c].wait_recv()
            for k in range(4):
                for i in range(n_i):
                    at = kept(c, i, k, 1)
                    both = qo[at[0], at[1], :] + pair_in[c, pl.ds((i * 4 + k) * n_rows, n_rows), :]
                    if k in (0, second[c]):
                        qo[at[0], at[1], :] = both
                    else:
                        total[c, k // 3, :, pl.ds(i * 128, 128)] = both.astype(BF16)
            for i in (1, 0):
                copy = remote(total.at[c, i], chip_in.at[c, i], chip_sem.at[l, c, i], peer[2 * first[c]])
                copy.start()
                chip.append(copy)

        def relay_chunk(c):
            chip[2 * c].wait_recv()
            for i in range(n_i):
                at, lanes = kept(c, i, second[c], 1), pl.ds(i * 128, 128)
                total[c, 2, :, lanes] = (qo[at[0], at[1], :] + chip_in[c, 1, :, lanes].astype(F32)).astype(BF16)
            copy = remote(total.at[c, 2], chip_in.at[c, 2], chip_sem.at[l, c, 2], peer[2 * second[c]])
            copy.start()
            relay.append(copy)

        for c in range(n_r):
            n, col = c * RS_CHUNK // CHUNK, c * RS_CHUNK % CHUNK
            if col == 0:
                ffn_copy(l, 2 * n_d + n).wait()
            y = dot(act[...], buf[ffn_at(l, (2 * n_d + n) * pad_width, width), pl.ds(col, RS_CHUNK)])
            y = y.reshape(4, 2, n_rows, RS_CHUNK)
            theirs, mine = (y[:, i].reshape(4 * n_rows, RS_CHUNK) for i in (1, 0))
            for i in range(n_i):
                outbox[c, pl.ds(i * 4 * n_rows, 4 * n_rows), :] = theirs[:, i * 128:(i + 1) * 128]
            copy = remote(outbox.at[c], pair_in.at[c], pair_sem.at[l, c], peer[1])
            copy.start()
            pair.append(copy)
            for i in range(n_i):
                at = kept(c, i, 0, 4)
                qo[at[0], at[1], :] = mine[:, i * 128:(i + 1) * 128]
            if c >= 2:
                reduce_chunk(c - 2)
        for c in (n_r - 2, n_r - 1):
            reduce_chunk(c)
        if l + 1 < n_layers:
            start(kv_copy(l + 1, b) for b in range(n_rows))
            start(wo_copy(l + 1, n) for n in range(n_d))
        else:
            start(head_copy(i) for i in range(HEAD_B, HEAD_A))
        for c in range(n_r):
            relay_chunk(c)
        for c in range(n_r):
            cols = pl.ds(c * RS_CHUNK, RS_CHUNK)
            chip[2 * c + 1].wait_recv()
            relay[c].wait_recv()
            at = [kept(c, i, 0, 1) for i in range(n_i)]
            y = jnp.concatenate([qo[t, r, :] for t, r in at], axis=1)
            for i in (0, 2):
                y = y + chip_in[c, i].astype(F32)
            x_cur[:, cols] = (x_cur[:, cols].astype(F32) + y).astype(BF16)
        for copy in sent + pair + chip + relay:
            copy.wait_send()

    hrows[0] = rms_norm(x_cur[...], gain_fin[...])
    rows[me] = hrows[0]
    peer[0] = me
    sends = gather(hrows.at[0], lambda j, k: rows.at[peer[j]], fin_sem)
    for copy in sends:
        copy.wait_send()
    for i in range(n_vocab):
        head_copy(i).wait()


def head_kernel(dims, rows, buf, out_hbm, tile, sem):
    d_model, vocab = dims
    n_vocab = vocab // CHUNK

    def out_copy(i, cols, slot):
        at = pl.ds(i * 2 * CHUNK if isinstance(i, int) else pl.multiple_of(i * 2 * CHUNK, 128), cols)
        return pltpu.make_async_copy(tile.at[slot, :, pl.ds(0, cols)], out_hbm.at[:, at], sem.at[slot])

    def weights(chunk):
        return buf[pl.ds(pl.multiple_of(head_chunk(chunk) * d_model, 128), d_model), :]

    def step(i, carry):
        half = lax.rem(i, 2) * 2

        @pl.when(i >= 2)
        def _():
            for h in (0, 1):
                out_copy(2 * i - 4 + h, 2 * CHUNK, half + h).wait()

        for c in range(4):
            tile[half + c // 2, :, pl.ds(c % 2 * CHUNK, CHUNK)] = dot(x, weights(4 * i + c))
        for h in (0, 1):
            out_copy(2 * i + h, 2 * CHUNK, half + h).start()
        return carry

    x = rows[...].reshape(-1, d_model)
    n_quads = n_vocab // 4
    lax.fori_loop(0, n_quads, step, 0)
    for i in range(max(n_quads - 2, 0), n_quads):
        for h in (0, 1):
            out_copy(2 * i + h, 2 * CHUNK, i % 2 * 2 + h).wait()
        if i == n_quads - 2 and n_vocab % 4:
            last = n_quads % 2 * 2
            tile[last, :, pl.ds(0, CHUNK)] = dot(x, weights(n_vocab - 1))
            out_copy(2 * n_quads, CHUNK, last).start()
    if n_vocab % 4:
        out_copy(2 * n_quads, CHUNK, n_quads % 2 * 2).wait()


def run_head(rows, buf, vocab):
    n_rows, d_model = rows.shape[0] * rows.shape[1], rows.shape[2]
    vmem = pl.BlockSpec(memory_space=pltpu.VMEM)
    rows, buf = (pltpu.with_memory_space_constraint(a, pltpu.VMEM) for a in (rows, buf))
    return pl.pallas_call(
        functools.partial(head_kernel, (d_model, vocab)),
        out_shape=jax.ShapeDtypeStruct((n_rows, vocab), F32),
        in_specs=[vmem, vmem],
        out_specs=pl.BlockSpec(memory_space=pl.ANY),
        scratch_shapes=[pltpu.VMEM((4, n_rows, 2 * CHUNK), F32), pltpu.SemaphoreType.DMA((4,))],
        compiler_params=pltpu.CompilerParams(vmem_limit_bytes=VMEM_LAYERS),
        name='head',
    )(rows, buf)


def run_layers(hidden, lengths, kv_t, gain_attn, w_q, w_o, gain_ffn, wg_t, wu_t, w_down, gain_fin, w_head):
    n_layers, n_rows, kv_width, seq_len = kv_t.shape
    d_model = hidden.shape[1]
    n_heads = w_q.shape[2] // kv_width
    width = w_down.shape[1]
    pad_width = round_up(width, 16)
    half, n_d, n_r = n_heads // 2, d_model // CHUNK, d_model // RS_CHUNK
    n_q = half * kv_width // CHUNK
    n_t = round_up(kv_width, 128) // 128
    slot_rows = max(n_q * d_model, n_rows * kv_width, n_d * half * LATENT, 3 * n_d * pad_width)
    dims = (n_layers, n_rows, d_model, n_heads, kv_width, seq_len, width, pad_width, slot_rows, w_head.shape[1])
    vmem, anys = pl.BlockSpec(memory_space=pltpu.VMEM), pl.BlockSpec(memory_space=pl.ANY)
    smem = pl.BlockSpec(memory_space=pltpu.SMEM)
    dma = pltpu.SemaphoreType.DMA
    scratch = [
        pltpu.VMEM((n_rows, d_model), BF16),
        pltpu.VMEM((2, n_rows, d_model), BF16),
        pltpu.VMEM((n_t, n_heads * n_rows, 128), F32),
        pltpu.VMEM((n_r, half * n_rows, 128), F32),
        pltpu.VMEM((2, GROUP, n_heads, seq_len), BF16),
        pltpu.VMEM((2, half, n_rows, LATENT), BF16),
        pltpu.VMEM((half, n_rows, LATENT), BF16),
        pltpu.VMEM((n_d, CHUNK // 128 * n_rows, 128), F32),
        pltpu.VMEM((NUM_DEV * n_rows, width), BF16),
        pltpu.VMEM((n_r, half * n_rows, 128), F32),
        pltpu.VMEM((n_r, 3, n_rows, RS_CHUNK), BF16),
        pltpu.VMEM((n_r, 3, n_rows, RS_CHUNK), BF16),
        dma((n_layers, n_q)), dma((n_layers, n_rows)), dma((n_layers, n_d)), dma((n_layers, 3 * n_d)),
        dma((n_layers, 2)), dma((n_layers, half // 2, 2)), dma((n_layers, 2)), dma((n_layers, n_d, 2)),
        dma((n_layers, 25, 2)), dma((n_layers, n_r, 2)), dma((n_layers, n_r, 3, 2)), dma((25, 2)), dma((w_head.shape[1] // CHUNK,)),
    ]
    return pl.pallas_call(
        functools.partial(layers_kernel, dims),
        out_shape=[pltpu.VMEM((NUM_DEV, n_rows, d_model), BF16), pltpu.VMEM((3 * slot_rows, CHUNK), BF16)],
        in_specs=[vmem, smem, vmem, vmem, vmem] + [anys] * 7,
        out_specs=[vmem, vmem],
        scratch_shapes=scratch,
        compiler_params=pltpu.CompilerParams(collective_id=0, has_side_effects=True, vmem_limit_bytes=VMEM_LAYERS),
        name='layers',
    )(hidden, lengths, gain_attn, gain_ffn, gain_fin.reshape(1, -1), kv_t, w_q, w_o, wg_t, wu_t, w_down, w_head)


def solution(mesh):
    row_axes = ('rep', 'dp')
    specs_in = (P(row_axes, None), P(row_axes), P(None, row_axes, None, None), P(), P(), P(), P(),
                P(None, None, 'dp'), P(None, None, 'dp'), P(None, 'dp', None), P(), P(None, 'dp'))

    def device_step(hidden, lengths, kv_cache, norm_attn, w_q, w_o, norm_ffn, w_gate, w_up, w_down, norm_final, w_head):
        rows, buf = run_layers(hidden, lengths, jnp.swapaxes(kv_cache, 2, 3), norm_attn, w_q, w_o, norm_ffn,
                               jnp.swapaxes(w_gate, 1, 2), jnp.swapaxes(w_up, 1, 2), w_down, norm_final, w_head)
        return run_head(rows, buf, w_head.shape[1])

    return jax.shard_map(device_step, mesh=mesh, in_specs=specs_in, out_specs=P('rep', 'dp'), check_vma=False)
```

```python
import functools

import jax
import jax.numpy as jnp
from jax import lax
from jax.experimental import pallas as pl
from jax.experimental.pallas import tpu as pltpu
from jax.sharding import PartitionSpec as P

LATENT = 512
QK_SCALE = 192 ** -0.5
NORM_EPS = 1e-6
MESH_ID = pl.DeviceIdType.MESH
NUM_DEV = 8
CHUNK = 512
GROUP = 8
HEAD_A, HEAD_B = 16, 9
VMEM_LAYERS = int(8.9 * 2**20)
BF16, F32 = jnp.bfloat16, jnp.float32


def rms_norm(x_rows, gain_vec):
    x_float = x_rows.astype(F32)
    inv_rms = lax.rsqrt(jnp.mean(x_float * x_float, axis=-1, keepdims=True) + NORM_EPS)
    return (x_float * inv_rms * gain_vec).astype(BF16)


def dot(a, b):
    return jnp.dot(a, b, preferred_element_type=F32)


def dot_nt(a, b):
    return lax.dot_general(a, b, (((1,), (1,)), ((), ())), preferred_element_type=F32)


def round_up(n, m):
    return (n + m - 1) // m * m


def head_chunk(i):
    return i + i // HEAD_A * 2


def cuts_of(width):
    return [(lo, min(lo + CHUNK, width)) for lo in range(0, width, CHUNK)]


def layers_kernel(dims, x_ref, len_ref, gain_attn, gain_ffn, gain_fin, kv_hbm, wq_hbm, wo_hbm, wg_hbm, wu_hbm, wd_hbm,
                  wh_hbm, rows, buf, x_cur, hrows, qo, outbox, p_buf, ol, ol_send, pr, act, pair_in, total, chip_in,
                  wq_sem, kv_sem, wo_sem, ffn_sem, h_sem, q_sem, o_sem, p_sem, ag_sem, pair_sem, chip_sem, fin_sem, head_sem):
    n_layers, n_rows, d_model, n_heads, kv_width, seq_len, width, pad_width, slot_rows, vocab = dims
    half = n_heads // 2
    q_cols = half * kv_width
    n_q, n_d = q_cols // CHUNK, d_model // CHUNK
    o_rows = half * LATENT
    n_t, n_j = round_up(kv_width, 128) // 128, CHUNK // 128
    cuts = cuts_of(width)
    n_vocab = vocab // CHUNK

    me = lax.axis_index('dp')
    core, x_pos, y_pos = me % 2, (me // 2) % 2, me // 4
    flip = lambda c, a, b: ((y_pos + b) % 2) * 4 + ((x_pos + a) % 2) * 2 + (core + c) % 2
    peer = {1: flip(1, 0, 0), 2: flip(0, 1, 0), 4: flip(0, 0, 1), 6: flip(0, 1, 1)}
    other = 1 - core

    def remote(src, dst, sems, dev):
        return pltpu.make_async_remote_copy(src_ref=src, dst_ref=dst, send_sem=sems.at[0], recv_sem=sems.at[1],
                                            device_id={'dp': dev}, device_id_type=MESH_ID)

    wq_at = lambda l, row, n: pl.ds(l % 3 * slot_rows + row, n)
    kv_at = lambda l, row, n: pl.ds((l + 1) % 3 * slot_rows + row, n)
    wo_at = lambda l, row, n: pl.ds((l + 2) % 3 * slot_rows + row, n)
    ffn_at = wq_at

    def wq_copy(l, n):
        cols = pl.ds(pl.multiple_of(core * q_cols + n * CHUNK, 128), CHUNK)
        return pltpu.make_async_copy(wq_hbm.at[l, :, cols], buf.at[wq_at(l, n * d_model, d_model)], wq_sem.at[l, n])

    def kv_copy(l, b):
        row = b * kv_width if isinstance(b, int) else pl.multiple_of(b * kv_width, 64)
        return pltpu.make_async_copy(kv_hbm.at[l, b], buf.at[kv_at(l, row, kv_width)], kv_sem.at[l, b])

    def wo_copy(l, n):
        src = wo_hbm.at[l, pl.ds(pl.multiple_of(core * o_rows, 128), o_rows), pl.ds(n * CHUNK, CHUNK)]
        return pltpu.make_async_copy(src, buf.at[wo_at(l, n * o_rows, o_rows)], wo_sem.at[l, n])

    def ffn_copy(l, i):
        src = (wg_hbm, wu_hbm, wd_hbm)[i // n_d]
        return pltpu.make_async_copy(src.at[l, :, pl.ds((i % n_d) * CHUNK, CHUNK)],
                                     buf.at[ffn_at(l, i * pad_width, width)], ffn_sem.at[l, i])

    def head_copy(i):
        row = head_chunk(i) * d_model
        return pltpu.make_async_copy(wh_hbm.at[:, pl.ds(i * CHUNK, CHUNK)], buf.at[pl.ds(row, d_model)], head_sem.at[i])

    def start(copies):
        for copy in copies:
            copy.start()

    def gather(own, block, sems):
        every, size = [], n_rows // 4
        chunk = lambda ref, c: ref.at[pl.ds(c * size, size)]

        def send(src, j, k):
            copy = remote(src, block(j, k), sems.at[len(every)], peer[k])
            copy.start()
            every.append(copy)
            return copy

        def send_chunk(src, c, j, k):
            copy = remote(chunk(src, c), chunk(block(j, k), c), sems.at[len(every)], peer[k])
            copy.start()
            every.append(copy)
            return copy

        x_order, y_order = (0, 1, 2, 3), (2, 3, 0, 1)
        near = {}
        for cx, cy in zip(x_order, y_order):
            near[2, cx] = send_chunk(own, cx, 0, 2)
            near[4, cy] = send_chunk(own, cy, 0, 4)
        arrivals = [send(own, 0, 1)]
        far = {}
        for i in range(4):
            for j, c in ((2, x_order[i]), (4, y_order[i])):
                near[j, c].wait_recv()
                if i < 2:
                    far[c] = send_chunk(block(j, 0), c, j, 6 - j)
                arrivals.append(send_chunk(block(j, 0), c, j, 1))
        for c in (0, 2, 1, 3):
            far[c].wait_recv()
            arrivals.append(send_chunk(block(6, 0), c, 6, 1))
        for copy in arrivals:
            copy.wait_recv()
        return every

    start(wq_copy(0, n) for n in range(n_q))
    x_cur[...] = x_ref[...]

    for l in range(n_layers):
        sent = []
        hrows[0] = rms_norm(x_cur[...], gain_attn[pl.ds(l, 1), :])
        if l == 0:
            barrier = pltpu.get_barrier_semaphore()
            for j in (1, 2, 4, 6):
                pl.semaphore_signal(barrier, inc=1, device_id={'dp': peer[j]}, device_id_type=MESH_ID)
            pl.semaphore_wait(barrier, 4)
        copy = remote(hrows.at[0], hrows.at[1], h_sem.at[l], peer[1])
        copy.start()
        sent.append(copy)
        copy.wait_recv()
        both_rows = hrows[...].reshape(2 * n_rows, d_model)
        prev, q_copies = None, []
        for first in range(0, n_q, 3):
            for n in range(first, first + 3):
                wq_copy(l, n).wait()
            if l == 0:
                per = -(-3 * n_rows // n_q)
                start(kv_copy(l, b) for b in range(first // 3 * per, min((first // 3 + 1) * per, n_rows)))
            weights = jnp.concatenate([buf[wq_at(l, n * d_model, d_model), :] for n in range(first, first + 3)], axis=1)
            wide = dot(both_rows, weights).astype(BF16).astype(F32)
            for n in range(first, first + 3):
                cur = wide[:, (n - first) * CHUNK:(n - first + 1) * CHUNK]
                if n >= 1:
                    h = n - 1
                    off = h * kv_width - h * CHUNK
                    q_head = jnp.concatenate([prev[:, off:], cur[:, :off + kv_width - CHUNK]], axis=1)
                    for j in range(n_t):
                        lanes = slice(j * 128, min((j + 1) * 128, kv_width))
                        keep = pl.ds(0, lanes.stop - lanes.start)
                        at = pl.ds(pl.multiple_of((core * half + h) * n_rows, n_rows), n_rows)
                        qo[j, at, keep] = q_head[:n_rows, lanes]
                        outbox[j, pl.ds(h * n_rows, n_rows), keep] = q_head[n_rows:, lanes]
                    if h % 2:
                        dst = qo.at[:, pl.ds(pl.multiple_of((core * half + h - 1) * n_rows, n_rows), 2 * n_rows)]
                        copy = remote(outbox.at[pl.ds(0, n_t), pl.ds((h - 1) * n_rows, 2 * n_rows)], dst, q_sem.at[l, h // 2], peer[1])
                        copy.start()
                        q_copies.append(copy)
                prev = cur
        if l == 0:
            start(wo_copy(l, n) for n in range(n_d))
        for copy in q_copies:
            copy.wait_recv()

        key_pos = lax.broadcasted_iota(jnp.int32, (n_heads, seq_len), 1)

        def scores(g, l=l):
            slot = lax.rem(g, 2)
            for i in range(GROUP):
                kv_copy(l, g * GROUP + i).wait()
            for i in range(GROUP):
                b = g * GROUP + i
                q = [qo[j, pl.ds(b, n_heads, stride=n_rows), :].astype(BF16) for j in range(n_t)]
                q = jnp.concatenate(q, axis=1)[:, :kv_width]
                row = pl.multiple_of(b * kv_width, 64)
                s = dot(q, buf[kv_at(l, row, kv_width), :]) * QK_SCALE
                s = jnp.where(key_pos < len_ref[b], s, -1e30)
                e = jnp.exp(s - jnp.max(s, axis=-1, keepdims=True))
                p_buf[slot, i] = (e / jnp.sum(e, axis=-1, keepdims=True)).astype(BF16)

        def contexts(g, l=l):
            slot = lax.rem(g, 2)
            for i in range(GROUP):
                b = g * GROUP + i
                row = pl.multiple_of(b * kv_width, 64)
                ctx = dot_nt(p_buf[slot, i], buf[kv_at(l, row, LATENT), :])
                for j in range(n_j):
                    qo[j, pl.ds(b, n_heads, stride=n_rows), :] = ctx[:, j * 128:(j + 1) * 128]

        n_groups = n_rows // GROUP
        scores(jnp.int32(0))

        def step(g, carry):
            scores(g)
            contexts(g - 1)
            return carry

        lax.fori_loop(1, n_groups, step, 0)
        contexts(jnp.int32(n_groups - 1))
        if l + 1 == n_layers:
            start(head_copy(i) for i in range(HEAD_A, n_vocab))

        for copy in q_copies:
            copy.wait_send()

        for h in range(half):
            at = pl.ds(pl.multiple_of((other * half + h) * n_rows, n_rows), n_rows)
            for j in range(n_j):
                ol_send[h, :, pl.ds(j * 128, 128)] = qo[j, at, :].astype(BF16)
        o_copy = remote(ol_send, ol.at[1], o_sem.at[l], peer[1])
        o_copy.start()
        sent.append(o_copy)
        start(ffn_copy(l, i) for i in range(3 * n_d))
        for h in range(half):
            at = pl.ds(pl.multiple_of((core * half + h) * n_rows, n_rows), n_rows)
            for j in range(n_j):
                ol[0, h, :, pl.ds(j * 128, 128)] = qo[j, at, :].astype(BF16)
        o_copy.wait_recv()
        p_copies, own = [], []
        context = jnp.concatenate([ol[:, h].reshape(2 * n_rows, LATENT) for h in range(half)], axis=1)
        for first in range(0, n_d, 2):
            for n in (first, first + 1):
                wo_copy(l, n).wait()
            weights = jnp.concatenate([buf[wo_at(l, n * o_rows, o_rows), :] for n in (first, first + 1)], axis=1)
            acc = dot(context, weights)
            for n in (first, first + 1):
                cols = slice((n - first) * CHUNK, (n - first + 1) * CHUNK)
                own.append(acc[:n_rows, cols])
                for j in range(n_j):
                    outbox[n, pl.ds(j * n_rows, n_rows), :] = acc[n_rows:, cols][:, j * 128:(j + 1) * 128]
                copy = remote(outbox.at[n, pl.ds(0, n_j * n_rows)], pr.at[n], p_sem.at[l, n], peer[1])
                copy.start()
                p_copies.append(copy)
        if l + 1 == n_layers:
            start(head_copy(i) for i in range(HEAD_B))
        for n in range(n_d):
            cols = pl.ds(n * CHUNK, CHUNK)
            p_copies[n].wait_recv()
            theirs = jnp.concatenate([pr[n, pl.ds(j * n_rows, n_rows), :] for j in range(n_j)], axis=1)
            x_cur[:, cols] = (x_cur[:, cols].astype(F32) + (own[n] + theirs)).astype(BF16)

        rows[0] = rms_norm(x_cur[...], gain_ffn[pl.ds(l, 1), :])
        row_sends = gather(rows.at[0], lambda j, k: rows.at[j ^ k], ag_sem.at[l])
        if l + 1 < n_layers:
            start(wq_copy(l + 1, n) for n in range(n_q))
        for i in range(2 * n_d):
            ffn_copy(l, i).wait()
        all_rows = rows[...].reshape(NUM_DEV * n_rows, d_model)
        for lo, hi in cuts:
            w_part = [jnp.concatenate([buf[ffn_at(l, (u * n_d + k) * pad_width + lo, hi - lo), :] for k in range(n_d)], axis=1)
                      for u in (0, 1)]
            gate = dot_nt(all_rows, w_part[0])
            up = dot_nt(all_rows, w_part[1])
            act[:, pl.ds(lo, hi - lo)] = (jax.nn.silu(gate) * up).astype(BF16)

        for copy in row_sends + p_copies:
            copy.wait_send()
        pair, chip = [], []

        def reduce_chunk(c):
            pair[c].wait_recv()
            for k in range(4):
                at = pl.ds((c * 4 + k) * n_rows, n_rows)
                for j in range(n_j):
                    lanes = pl.ds(j * 128, 128)
                    both = qo[j, at, :] + pair_in[2 * c + j // 2, pl.ds((j % 2 * 4 + k) * n_rows, n_rows), :]
                    if k == 0:
                        qo[j, at, :] = both
                    else:
                        total[c, k - 1, :, lanes] = both.astype(BF16)
            for k in (3, 1, 2):
                copy = remote(total.at[c, k - 1], chip_in.at[c, k - 1], chip_sem.at[l, c, k - 1], peer[2 * k])
                copy.start()
                chip.append(copy)

        for c in range(n_d):
            ffn_copy(l, 2 * n_d + c).wait()
            y = dot(act[...], buf[ffn_at(l, (2 * n_d + c) * pad_width, width), :])
            y = y.reshape(4, 2, n_rows, CHUNK)
            theirs = y[:, 1].reshape(4 * n_rows, CHUNK)
            for j in range(n_j):
                outbox[2 * c + j // 2, pl.ds(j % 2 * 4 * n_rows, 4 * n_rows), :] = theirs[:, j * 128:(j + 1) * 128]
            mine = y[:, 0].reshape(4 * n_rows, CHUNK)
            for j in range(n_j):
                qo[j, pl.ds(c * 4 * n_rows, 4 * n_rows), :] = mine[:, j * 128:(j + 1) * 128]
            copy = remote(outbox.at[pl.ds(2 * c, 2)], pair_in.at[pl.ds(2 * c, 2)], pair_sem.at[l, c], peer[1])
            copy.start()
            pair.append(copy)
            if c >= 1:
                reduce_chunk(c - 1)
        reduce_chunk(n_d - 1)
        if l + 1 < n_layers:
            start(kv_copy(l + 1, b) for b in range(n_rows))
            start(wo_copy(l + 1, n) for n in range(n_d))
        else:
            start(head_copy(i) for i in range(HEAD_B, HEAD_A))
        for c in range(n_d):
            cols = pl.ds(c * CHUNK, CHUNK)
            for copy in chip[3 * c:3 * c + 3]:
                copy.wait_recv()
            y = jnp.concatenate([qo[j, pl.ds(c * 4 * n_rows, n_rows), :] for j in range(n_j)], axis=1)
            for k in range(3):
                y = y + chip_in[c, k].astype(F32)
            x_cur[:, cols] = (x_cur[:, cols].astype(F32) + y).astype(BF16)
        for copy in sent + pair + chip:
            copy.wait_send()

    hrows[0] = rms_norm(x_cur[...], gain_fin[...])
    rows[me] = hrows[0]
    peer[0] = me
    sends = gather(hrows.at[0], lambda j, k: rows.at[peer[j]], fin_sem)
    for copy in sends:
        copy.wait_send()
    for i in range(n_vocab):
        head_copy(i).wait()


def head_kernel(dims, rows, buf, out_hbm, tile, sem):
    d_model, vocab = dims
    n_vocab = vocab // CHUNK

    def out_copy(i, cols, slot):
        at = pl.ds(i * 2 * CHUNK if isinstance(i, int) else pl.multiple_of(i * 2 * CHUNK, 128), cols)
        return pltpu.make_async_copy(tile.at[slot, :, pl.ds(0, cols)], out_hbm.at[:, at], sem.at[slot])

    def weights(chunk):
        return buf[pl.ds(pl.multiple_of(head_chunk(chunk) * d_model, 128), d_model), :]

    def step(i, carry):
        half = lax.rem(i, 2) * 2

        @pl.when(i >= 2)
        def _():
            for h in (0, 1):
                out_copy(2 * i - 4 + h, 2 * CHUNK, half + h).wait()

        for c in range(4):
            tile[half + c // 2, :, pl.ds(c % 2 * CHUNK, CHUNK)] = dot(x, weights(4 * i + c))
        for h in (0, 1):
            out_copy(2 * i + h, 2 * CHUNK, half + h).start()
        return carry

    x = rows[...].reshape(-1, d_model)
    n_quads = n_vocab // 4
    lax.fori_loop(0, n_quads, step, 0)
    for i in range(max(n_quads - 2, 0), n_quads):
        for h in (0, 1):
            out_copy(2 * i + h, 2 * CHUNK, i % 2 * 2 + h).wait()
        if i == n_quads - 2 and n_vocab % 4:
            last = n_quads % 2 * 2
            tile[last, :, pl.ds(0, CHUNK)] = dot(x, weights(n_vocab - 1))
            out_copy(2 * n_quads, CHUNK, last).start()
    if n_vocab % 4:
        out_copy(2 * n_quads, CHUNK, n_quads % 2 * 2).wait()


def run_head(rows, buf, vocab):
    n_rows, d_model = rows.shape[0] * rows.shape[1], rows.shape[2]
    vmem = pl.BlockSpec(memory_space=pltpu.VMEM)
    rows, buf = (pltpu.with_memory_space_constraint(a, pltpu.VMEM) for a in (rows, buf))
    return pl.pallas_call(
        functools.partial(head_kernel, (d_model, vocab)),
        out_shape=jax.ShapeDtypeStruct((n_rows, vocab), F32),
        in_specs=[vmem, vmem],
        out_specs=pl.BlockSpec(memory_space=pl.ANY),
        scratch_shapes=[pltpu.VMEM((4, n_rows, 2 * CHUNK), F32), pltpu.SemaphoreType.DMA((4,))],
        compiler_params=pltpu.CompilerParams(vmem_limit_bytes=VMEM_LAYERS),
        name='head',
    )(rows, buf)


def run_layers(hidden, lengths, kv_t, gain_attn, w_q, w_o, gain_ffn, wg_t, wu_t, w_down, gain_fin, w_head):
    n_layers, n_rows, kv_width, seq_len = kv_t.shape
    d_model = hidden.shape[1]
    n_heads = w_q.shape[2] // kv_width
    width = w_down.shape[1]
    pad_width = round_up(width, 16)
    half, n_d = n_heads // 2, d_model // CHUNK
    n_q = half * kv_width // CHUNK
    n_t = round_up(kv_width, 128) // 128
    slot_rows = max(n_q * d_model, n_rows * kv_width, n_d * half * LATENT, 3 * n_d * pad_width)
    dims = (n_layers, n_rows, d_model, n_heads, kv_width, seq_len, width, pad_width, slot_rows, w_head.shape[1])
    vmem, anys = pl.BlockSpec(memory_space=pltpu.VMEM), pl.BlockSpec(memory_space=pl.ANY)
    smem = pl.BlockSpec(memory_space=pltpu.SMEM)
    dma = pltpu.SemaphoreType.DMA
    scratch = [
        pltpu.VMEM((n_rows, d_model), BF16),
        pltpu.VMEM((2, n_rows, d_model), BF16),
        pltpu.VMEM((n_t, n_heads * n_rows, 128), F32),
        pltpu.VMEM((8, half * n_rows, 128), F32),
        pltpu.VMEM((2, GROUP, n_heads, seq_len), BF16),
        pltpu.VMEM((2, half, n_rows, LATENT), BF16),
        pltpu.VMEM((half, n_rows, LATENT), BF16),
        pltpu.VMEM((n_d, CHUNK // 128 * n_rows, 128), F32),
        pltpu.VMEM((NUM_DEV * n_rows, width), BF16),
        pltpu.VMEM((8, half * n_rows, 128), F32),
        pltpu.VMEM((n_d, 3, n_rows, CHUNK), BF16),
        pltpu.VMEM((n_d, 3, n_rows, CHUNK), BF16),
        dma((n_layers, n_q)), dma((n_layers, n_rows)), dma((n_layers, n_d)), dma((n_layers, 3 * n_d)),
        dma((n_layers, 2)), dma((n_layers, half // 2, 2)), dma((n_layers, 2)), dma((n_layers, n_d, 2)),
        dma((n_layers, 25, 2)), dma((n_layers, n_d, 2)), dma((n_layers, n_d, 3, 2)), dma((25, 2)), dma((w_head.shape[1] // CHUNK,)),
    ]
    return pl.pallas_call(
        functools.partial(layers_kernel, dims),
        out_shape=[pltpu.VMEM((NUM_DEV, n_rows, d_model), BF16), pltpu.VMEM((3 * slot_rows, CHUNK), BF16)],
        in_specs=[vmem, smem, vmem, vmem, vmem] + [anys] * 7,
        out_specs=[vmem, vmem],
        scratch_shapes=scratch,
        compiler_params=pltpu.CompilerParams(collective_id=0, has_side_effects=True, vmem_limit_bytes=VMEM_LAYERS),
        name='layers',
    )(hidden, lengths, gain_attn, gain_ffn, gain_fin.reshape(1, -1), kv_t, w_q, w_o, wg_t, wu_t, w_down, w_head)


def solution(mesh):
    row_axes = ('rep', 'dp')
    specs_in = (P(row_axes, None), P(row_axes), P(None, row_axes, None, None), P(), P(), P(), P(),
                P(None, None, 'dp'), P(None, None, 'dp'), P(None, 'dp', None), P(), P(None, 'dp'))

    def device_step(hidden, lengths, kv_cache, norm_attn, w_q, w_o, norm_ffn, w_gate, w_up, w_down, norm_final, w_head):
        rows, buf = run_layers(hidden, lengths, jnp.swapaxes(kv_cache, 2, 3), norm_attn, w_q, w_o, norm_ffn,
                               jnp.swapaxes(w_gate, 1, 2), jnp.swapaxes(w_up, 1, 2), w_down, norm_final, w_head)
        return run_head(rows, buf, w_head.shape[1])

    return jax.shard_map(device_step, mesh=mesh, in_specs=specs_in, out_specs=P('rep', 'dp'), check_vma=False)
```

```python
import functools

import jax
import jax.numpy as jnp
from jax import lax
from jax.experimental import pallas as pl
from jax.experimental.pallas import tpu as pltpu
from jax.sharding import PartitionSpec as P

LATENT = 512
QK_SCALE = 192 ** -0.5
NORM_EPS = 1e-6
MESH_ID = pl.DeviceIdType.MESH
NUM_DEV = 8
CHUNK = 512
GROUP = 8
HEAD_A, HEAD_B = 16, 9
VMEM_LAYERS = int(8.9 * 2**20)
BF16, F32 = jnp.bfloat16, jnp.float32


def rms_norm(x_rows, gain_vec):
    x_float = x_rows.astype(F32)
    inv_rms = lax.rsqrt(jnp.mean(x_float * x_float, axis=-1, keepdims=True) + NORM_EPS)
    return (x_float * inv_rms * gain_vec).astype(BF16)


def dot(a, b):
    return jnp.dot(a, b, preferred_element_type=F32)


def dot_nt(a, b):
    return lax.dot_general(a, b, (((1,), (1,)), ((), ())), preferred_element_type=F32)


def round_up(n, m):
    return (n + m - 1) // m * m


def head_chunk(i):
    return i + i // HEAD_A * 2


def cuts_of(width):
    return [(lo, min(lo + CHUNK, width)) for lo in range(0, width, CHUNK)]


def layers_kernel(dims, x_hbm, len_hbm, gain_attn_hbm, gain_ffn_hbm, gain_fin_hbm, kv_hbm, wq_hbm, wo_hbm, wg_hbm, wu_hbm, wd_hbm,
                  wh_hbm, rows, buf, x_cur, hrows, qo, outbox, p_buf, ol, ol_send, pr, act, pair_in, total, chip_in,
                  wq_sem, kv_sem, wo_sem, ffn_sem, h_sem, q_sem, o_sem, p_sem, ag_sem, pair_sem, chip_sem, fin_sem, head_sem,
                  len_ref, gain_attn, gain_ffn, gain_fin, in_sem):
    n_layers, n_rows, d_model, n_heads, kv_width, seq_len, width, pad_width, slot_rows, vocab = dims
    half = n_heads // 2
    q_cols = half * kv_width
    n_q, n_d = q_cols // CHUNK, d_model // CHUNK
    o_rows = half * LATENT
    n_t, n_j = round_up(kv_width, 128) // 128, CHUNK // 128
    cuts = cuts_of(width)
    n_vocab = vocab // CHUNK

    me = lax.axis_index('dp')
    core, x_pos, y_pos = me % 2, (me // 2) % 2, me // 4
    flip = lambda c, a, b: ((y_pos + b) % 2) * 4 + ((x_pos + a) % 2) * 2 + (core + c) % 2
    peer = {1: flip(1, 0, 0), 2: flip(0, 1, 0), 4: flip(0, 0, 1), 6: flip(0, 1, 1)}
    other = 1 - core

    def remote(src, dst, sems, dev):
        return pltpu.make_async_remote_copy(src_ref=src, dst_ref=dst, send_sem=sems.at[0], recv_sem=sems.at[1],
                                            device_id={'dp': dev}, device_id_type=MESH_ID)

    wq_at = lambda l, row, n: pl.ds(l % 3 * slot_rows + row, n)
    kv_at = lambda l, row, n: pl.ds((l + 1) % 3 * slot_rows + row, n)
    wo_at = lambda l, row, n: pl.ds((l + 2) % 3 * slot_rows + row, n)
    ffn_at = wq_at

    def wq_copy(l, n):
        cols = pl.ds(pl.multiple_of(core * q_cols + n * CHUNK, 128), CHUNK)
        return pltpu.make_async_copy(wq_hbm.at[l, :, cols], buf.at[wq_at(l, n * d_model, d_model)], wq_sem.at[l, n])

    def kv_copy(l, b):
        row = b * kv_width if isinstance(b, int) else pl.multiple_of(b * kv_width, 64)
        return pltpu.make_async_copy(kv_hbm.at[l, b], buf.at[kv_at(l, row, kv_width)], kv_sem.at[l, b])

    def wo_copy(l, n):
        src = wo_hbm.at[l, pl.ds(pl.multiple_of(core * o_rows, 128), o_rows), pl.ds(n * CHUNK, CHUNK)]
        return pltpu.make_async_copy(src, buf.at[wo_at(l, n * o_rows, o_rows)], wo_sem.at[l, n])

    def ffn_copy(l, i):
        src = (wg_hbm, wu_hbm, wd_hbm)[i // n_d]
        return pltpu.make_async_copy(src.at[l, :, pl.ds((i % n_d) * CHUNK, CHUNK)],
                                     buf.at[ffn_at(l, i * pad_width, width)], ffn_sem.at[l, i])

    def head_copy(i):
        row = head_chunk(i) * d_model
        return pltpu.make_async_copy(wh_hbm.at[:, pl.ds(i * CHUNK, CHUNK)], buf.at[pl.ds(row, d_model)], head_sem.at[i])

    def start(copies):
        for copy in copies:
            copy.start()

    def gather(own, block, sems):
        every, size = [], n_rows // 4
        chunk = lambda ref, c: ref.at[pl.ds(c * size, size)]

        def send(src, j, k):
            copy = remote(src, block(j, k), sems.at[len(every)], peer[k])
            copy.start()
            every.append(copy)
            return copy

        def send_chunk(src, c, j, k):
            copy = remote(chunk(src, c), chunk(block(j, k), c), sems.at[len(every)], peer[k])
            copy.start()
            every.append(copy)
            return copy

        x_order, y_order = (0, 1, 2, 3), (2, 3, 0, 1)
        near = {}
        for cx, cy in zip(x_order, y_order):
            near[2, cx] = send_chunk(own, cx, 0, 2)
            near[4, cy] = send_chunk(own, cy, 0, 4)
        arrivals = [send(own, 0, 1)]
        far = {}
        for i in range(4):
            for j, c in ((2, x_order[i]), (4, y_order[i])):
                near[j, c].wait_recv()
                if i < 2:
                    far[c] = send_chunk(block(j, 0), c, j, 6 - j)
                arrivals.append(send_chunk(block(j, 0), c, j, 1))
        for c in (0, 2, 1, 3):
            far[c].wait_recv()
            arrivals.append(send_chunk(block(6, 0), c, 6, 1))
        for copy in arrivals:
            copy.wait_recv()
        return every

    start(wq_copy(0, n) for n in range(n_q))
    small = [pltpu.make_async_copy(src, dst, in_sem.at[i]) for i, (src, dst) in enumerate(
        ((x_hbm, x_cur), (gain_attn_hbm, gain_attn), (gain_ffn_hbm, gain_ffn), (gain_fin_hbm, gain_fin), (len_hbm, len_ref)))]
    start(small)
    for copy in small:
        copy.wait()

    for l in range(n_layers):
        sent = []
        hrows[0] = rms_norm(x_cur[...], gain_attn[pl.ds(l, 1), :])
        if l == 0:
            barrier = pltpu.get_barrier_semaphore()
            for j in (1, 2, 4, 6):
                pl.semaphore_signal(barrier, inc=1, device_id={'dp': peer[j]}, device_id_type=MESH_ID)
            pl.semaphore_wait(barrier, 4)
        copy = remote(hrows.at[0], hrows.at[1], h_sem.at[l], peer[1])
        copy.start()
        sent.append(copy)
        copy.wait_recv()
        both_rows = hrows[...].reshape(2 * n_rows, d_model)
        prev, q_copies = None, []
        bounds = [(i, min(i + 3, n_q)) for i in range(0, n_q, 3)]
        if l == 0:
            bounds[-1:] = [(n_q - 3, n_q - 1), (n_q - 1, n_q)]
        for first, stop in bounds:
            for n in range(first, stop):
                wq_copy(l, n).wait()
            if l == 0:
                start(kv_copy(l, b) for b in range(first * n_rows // n_q, stop * n_rows // n_q))
            weights = jnp.concatenate([buf[wq_at(l, n * d_model, d_model), :] for n in range(first, stop)], axis=1)
            wide = dot(both_rows, weights).astype(BF16).astype(F32)
            for n in range(first, stop):
                cur = wide[:, (n - first) * CHUNK:(n - first + 1) * CHUNK]
                if n >= 1:
                    h = n - 1
                    off = h * kv_width - h * CHUNK
                    q_head = jnp.concatenate([prev[:, off:], cur[:, :off + kv_width - CHUNK]], axis=1)
                    for j in range(n_t):
                        lanes = slice(j * 128, min((j + 1) * 128, kv_width))
                        keep = pl.ds(0, lanes.stop - lanes.start)
                        at = pl.ds(pl.multiple_of((core * half + h) * n_rows, n_rows), n_rows)
                        qo[j, at, keep] = q_head[:n_rows, lanes]
                        outbox[j, pl.ds(h * n_rows, n_rows), keep] = q_head[n_rows:, lanes]
                    if h % 2:
                        dst = qo.at[:, pl.ds(pl.multiple_of((core * half + h - 1) * n_rows, n_rows), 2 * n_rows)]
                        copy = remote(outbox.at[pl.ds(0, n_t), pl.ds((h - 1) * n_rows, 2 * n_rows)], dst, q_sem.at[l, h // 2], peer[1])
                        copy.start()
                        q_copies.append(copy)
                prev = cur
        if l == 0:
            start(wo_copy(l, n) for n in range(n_d))
        for copy in q_copies:
            copy.wait_recv()

        key_pos = lax.broadcasted_iota(jnp.int32, (n_heads, seq_len), 1)

        def scores(g, l=l):
            slot = lax.rem(g, 2)
            for i in range(GROUP):
                kv_copy(l, g * GROUP + i).wait()
            for i in range(GROUP):
                b = g * GROUP + i
                q = [qo[j, pl.ds(b, n_heads, stride=n_rows), :].astype(BF16) for j in range(n_t)]
                q = jnp.concatenate(q, axis=1)[:, :kv_width]
                row = pl.multiple_of(b * kv_width, 64)
                s = dot(q, buf[kv_at(l, row, kv_width), :]) * QK_SCALE
                s = jnp.where(key_pos < len_ref[0, b], s, -1e30)
                e = jnp.exp(s - jnp.max(s, axis=-1, keepdims=True))
                p_buf[slot, i] = (e / jnp.sum(e, axis=-1, keepdims=True)).astype(BF16)

        def contexts(g, l=l):
            slot = lax.rem(g, 2)
            for i in range(GROUP):
                b = g * GROUP + i
                row = pl.multiple_of(b * kv_width, 64)
                ctx = dot_nt(p_buf[slot, i], buf[kv_at(l, row, LATENT), :])
                for j in range(n_j):
                    qo[j, pl.ds(b, n_heads, stride=n_rows), :] = ctx[:, j * 128:(j + 1) * 128]

        n_groups = n_rows // GROUP
        scores(jnp.int32(0))

        def step(g, carry):
            scores(g)
            contexts(g - 1)
            return carry

        lax.fori_loop(1, n_groups, step, 0)
        contexts(jnp.int32(n_groups - 1))
        if l + 1 == n_layers:
            start(head_copy(i) for i in range(HEAD_A, n_vocab))

        for copy in q_copies:
            copy.wait_send()

        for h in range(half):
            at = pl.ds(pl.multiple_of((other * half + h) * n_rows, n_rows), n_rows)
            for j in range(n_j):
                ol_send[h, :, pl.ds(j * 128, 128)] = qo[j, at, :].astype(BF16)
        o_copy = remote(ol_send, ol.at[1], o_sem.at[l], peer[1])
        o_copy.start()
        sent.append(o_copy)
        start(ffn_copy(l, i) for i in range(3 * n_d))
        for h in range(half):
            at = pl.ds(pl.multiple_of((core * half + h) * n_rows, n_rows), n_rows)
            for j in range(n_j):
                ol[0, h, :, pl.ds(j * 128, 128)] = qo[j, at, :].astype(BF16)
        o_copy.wait_recv()
        p_copies, own = [], []
        context = jnp.concatenate([ol[:, h].reshape(2 * n_rows, LATENT) for h in range(half)], axis=1)
        for first in range(0, n_d, 2):
            for n in (first, first + 1):
                wo_copy(l, n).wait()
            weights = jnp.concatenate([buf[wo_at(l, n * o_rows, o_rows), :] for n in (first, first + 1)], axis=1)
            acc = dot(context, weights)
            for n in (first, first + 1):
                cols = slice((n - first) * CHUNK, (n - first + 1) * CHUNK)
                own.append(acc[:n_rows, cols])
                for j in range(n_j):
                    outbox[n, pl.ds(j * n_rows, n_rows), :] = acc[n_rows:, cols][:, j * 128:(j + 1) * 128]
                copy = remote(outbox.at[n, pl.ds(0, n_j * n_rows)], pr.at[n], p_sem.at[l, n], peer[1])
                copy.start()
                p_copies.append(copy)
        if l + 1 == n_layers:
            start(head_copy(i) for i in range(HEAD_B))
        for n in range(n_d):
            cols = pl.ds(n * CHUNK, CHUNK)
            p_copies[n].wait_recv()
            theirs = jnp.concatenate([pr[n, pl.ds(j * n_rows, n_rows), :] for j in range(n_j)], axis=1)
            x_cur[:, cols] = (x_cur[:, cols].astype(F32) + (own[n] + theirs)).astype(BF16)

        rows[0] = rms_norm(x_cur[...], gain_ffn[pl.ds(l, 1), :])
        row_sends = gather(rows.at[0], lambda j, k: rows.at[j ^ k], ag_sem.at[l])
        if l + 1 < n_layers:
            start(wq_copy(l + 1, n) for n in range(n_q))
        for i in range(2 * n_d):
            ffn_copy(l, i).wait()
        all_rows = rows[...].reshape(NUM_DEV * n_rows, d_model)
        for lo, hi in cuts:
            w_part = [jnp.concatenate([buf[ffn_at(l, (u * n_d + k) * pad_width + lo, hi - lo), :] for k in range(n_d)], axis=1)
                      for u in (0, 1)]
            gate = dot_nt(all_rows, w_part[0])
            up = dot_nt(all_rows, w_part[1])
            act[:, pl.ds(lo, hi - lo)] = (jax.nn.silu(gate) * up).astype(BF16)

        for copy in row_sends + p_copies:
            copy.wait_send()
        pair, chip = [], []

        def reduce_chunk(c):
            pair[c].wait_recv()
            for k in range(4):
                at = pl.ds((c * 4 + k) * n_rows, n_rows)
                for j in range(n_j):
                    lanes = pl.ds(j * 128, 128)
                    both = qo[j, at, :] + pair_in[2 * c + j // 2, pl.ds((j % 2 * 4 + k) * n_rows, n_rows), :]
                    if k == 0:
                        qo[j, at, :] = both
                    else:
                        total[c, k - 1, :, lanes] = both.astype(BF16)
            for k in (3, 1, 2):
                copy = remote(total.at[c, k - 1], chip_in.at[c, k - 1], chip_sem.at[l, c, k - 1], peer[2 * k])
                copy.start()
                chip.append(copy)

        for c in range(n_d):
            ffn_copy(l, 2 * n_d + c).wait()
            y = dot(act[...], buf[ffn_at(l, (2 * n_d + c) * pad_width, width), :])
            y = y.reshape(4, 2, n_rows, CHUNK)
            theirs = y[:, 1].reshape(4 * n_rows, CHUNK)
            for j in range(n_j):
                outbox[2 * c + j // 2, pl.ds(j % 2 * 4 * n_rows, 4 * n_rows), :] = theirs[:, j * 128:(j + 1) * 128]
            mine = y[:, 0].reshape(4 * n_rows, CHUNK)
            for j in range(n_j):
                qo[j, pl.ds(c * 4 * n_rows, 4 * n_rows), :] = mine[:, j * 128:(j + 1) * 128]
            copy = remote(outbox.at[pl.ds(2 * c, 2)], pair_in.at[pl.ds(2 * c, 2)], pair_sem.at[l, c], peer[1])
            copy.start()
            pair.append(copy)
            if c >= 1:
                reduce_chunk(c - 1)
        reduce_chunk(n_d - 1)
        if l + 1 < n_layers:
            start(kv_copy(l + 1, b) for b in range(n_rows))
            start(wo_copy(l + 1, n) for n in range(n_d))
        else:
            start(head_copy(i) for i in range(HEAD_B, HEAD_A))
        for c in range(n_d):
            cols = pl.ds(c * CHUNK, CHUNK)
            for copy in chip[3 * c:3 * c + 3]:
                copy.wait_recv()
            y = jnp.concatenate([qo[j, pl.ds(c * 4 * n_rows, n_rows), :] for j in range(n_j)], axis=1)
            for k in range(3):
                y = y + chip_in[c, k].astype(F32)
            x_cur[:, cols] = (x_cur[:, cols].astype(F32) + y).astype(BF16)
        for copy in sent + pair + chip:
            copy.wait_send()

    hrows[0] = rms_norm(x_cur[...], gain_fin[...])
    rows[me] = hrows[0]
    peer[0] = me
    sends = gather(hrows.at[0], lambda j, k: rows.at[peer[j]], fin_sem)
    for copy in sends:
        copy.wait_send()
    for i in range(n_vocab):
        head_copy(i).wait()


def head_kernel(dims, rows, buf, out_hbm, tile, sem):
    d_model, vocab = dims
    n_vocab = vocab // CHUNK

    def out_copy(i, cols, slot):
        at = pl.ds(i * 2 * CHUNK if isinstance(i, int) else pl.multiple_of(i * 2 * CHUNK, 128), cols)
        return pltpu.make_async_copy(tile.at[slot, :, pl.ds(0, cols)], out_hbm.at[:, at], sem.at[slot])

    def weights(chunk):
        return buf[pl.ds(pl.multiple_of(head_chunk(chunk) * d_model, 128), d_model), :]

    def step(i, carry):
        half = lax.rem(i, 2) * 2

        @pl.when(i >= 2)
        def _():
            for h in (0, 1):
                out_copy(2 * i - 4 + h, 2 * CHUNK, half + h).wait()

        for c in range(4):
            tile[half + c // 2, :, pl.ds(c % 2 * CHUNK, CHUNK)] = dot(x, weights(4 * i + c))
        for h in (0, 1):
            out_copy(2 * i + h, 2 * CHUNK, half + h).start()
        return carry

    x = rows[...].reshape(-1, d_model)
    n_quads = n_vocab // 4
    lax.fori_loop(0, n_quads, step, 0)
    for i in range(max(n_quads - 2, 0), n_quads):
        for h in (0, 1):
            out_copy(2 * i + h, 2 * CHUNK, i % 2 * 2 + h).wait()
        if i == n_quads - 2 and n_vocab % 4:
            last = n_quads % 2 * 2
            tile[last, :, pl.ds(0, CHUNK)] = dot(x, weights(n_vocab - 1))
            out_copy(2 * n_quads, CHUNK, last).start()
    if n_vocab % 4:
        out_copy(2 * n_quads, CHUNK, n_quads % 2 * 2).wait()


def run_head(rows, buf, vocab):
    n_rows, d_model = rows.shape[0] * rows.shape[1], rows.shape[2]
    vmem = pl.BlockSpec(memory_space=pltpu.VMEM)
    rows, buf = (pltpu.with_memory_space_constraint(a, pltpu.VMEM) for a in (rows, buf))
    return pl.pallas_call(
        functools.partial(head_kernel, (d_model, vocab)),
        out_shape=jax.ShapeDtypeStruct((n_rows, vocab), F32),
        in_specs=[vmem, vmem],
        out_specs=pl.BlockSpec(memory_space=pl.ANY),
        scratch_shapes=[pltpu.VMEM((4, n_rows, 2 * CHUNK), F32), pltpu.SemaphoreType.DMA((4,))],
        compiler_params=pltpu.CompilerParams(vmem_limit_bytes=VMEM_LAYERS),
        name='head',
    )(rows, buf)


def run_layers(hidden, lengths, kv_t, gain_attn, w_q, w_o, gain_ffn, wg_t, wu_t, w_down, gain_fin, w_head):
    n_layers, n_rows, kv_width, seq_len = kv_t.shape
    d_model = hidden.shape[1]
    n_heads = w_q.shape[2] // kv_width
    width = w_down.shape[1]
    pad_width = round_up(width, 16)
    half, n_d = n_heads // 2, d_model // CHUNK
    n_q = half * kv_width // CHUNK
    n_t = round_up(kv_width, 128) // 128
    slot_rows = max(n_q * d_model, n_rows * kv_width, n_d * half * LATENT, 3 * n_d * pad_width)
    dims = (n_layers, n_rows, d_model, n_heads, kv_width, seq_len, width, pad_width, slot_rows, w_head.shape[1])
    vmem, anys = pl.BlockSpec(memory_space=pltpu.VMEM), pl.BlockSpec(memory_space=pl.ANY)
    dma = pltpu.SemaphoreType.DMA
    scratch = [
        pltpu.VMEM((n_rows, d_model), BF16),
        pltpu.VMEM((2, n_rows, d_model), BF16),
        pltpu.VMEM((n_t, n_heads * n_rows, 128), F32),
        pltpu.VMEM((8, half * n_rows, 128), F32),
        pltpu.VMEM((2, GROUP, n_heads, seq_len), BF16),
        pltpu.VMEM((2, half, n_rows, LATENT), BF16),
        pltpu.VMEM((half, n_rows, LATENT), BF16),
        pltpu.VMEM((n_d, CHUNK // 128 * n_rows, 128), F32),
        pltpu.VMEM((NUM_DEV * n_rows, width), BF16),
        pltpu.VMEM((8, half * n_rows, 128), F32),
        pltpu.VMEM((n_d, 3, n_rows, CHUNK), BF16),
        pltpu.VMEM((n_d, 3, n_rows, CHUNK), BF16),
        dma((n_layers, n_q)), dma((n_layers, n_rows)), dma((n_layers, n_d)), dma((n_layers, 3 * n_d)),
        dma((n_layers, 2)), dma((n_layers, half // 2, 2)), dma((n_layers, 2)), dma((n_layers, n_d, 2)),
        dma((n_layers, 25, 2)), dma((n_layers, n_d, 2)), dma((n_layers, n_d, 3, 2)), dma((25, 2)), dma((w_head.shape[1] // CHUNK,)),
        pltpu.SMEM((1, n_rows), jnp.int32), pltpu.VMEM((n_layers, d_model), F32), pltpu.VMEM((n_layers, d_model), F32),
        pltpu.VMEM((1, d_model), F32), dma((5,)),
    ]
    return pl.pallas_call(
        functools.partial(layers_kernel, dims),
        out_shape=[pltpu.VMEM((NUM_DEV, n_rows, d_model), BF16), pltpu.VMEM((3 * slot_rows, CHUNK), BF16)],
        in_specs=[anys] * 12,
        out_specs=[vmem, vmem],
        scratch_shapes=scratch,
        compiler_params=pltpu.CompilerParams(collective_id=0, has_side_effects=True, vmem_limit_bytes=VMEM_LAYERS),
        name='layers',
    )(hidden, lengths.reshape(1, -1), gain_attn, gain_ffn, gain_fin.reshape(1, -1), kv_t, w_q, w_o, wg_t, wu_t, w_down, w_head)


def solution(mesh):
    row_axes = ('rep', 'dp')
    specs_in = (P(row_axes, None), P(row_axes), P(None, row_axes, None, None), P(), P(), P(), P(),
                P(None, None, 'dp'), P(None, None, 'dp'), P(None, 'dp', None), P(), P(None, 'dp'))

    def device_step(hidden, lengths, kv_cache, norm_attn, w_q, w_o, norm_ffn, w_gate, w_up, w_down, norm_final, w_head):
        rows, buf = run_layers(hidden, lengths, jnp.swapaxes(kv_cache, 2, 3), norm_attn, w_q, w_o, norm_ffn,
                               jnp.swapaxes(w_gate, 1, 2), jnp.swapaxes(w_up, 1, 2), w_down, norm_final, w_head)
        return run_head(rows, buf, w_head.shape[1])

    return jax.shard_map(device_step, mesh=mesh, in_specs=specs_in, out_specs=P('rep', 'dp'), check_vma=False)
```

```python
import functools

import jax
import jax.numpy as jnp
from jax import lax
from jax.experimental import pallas as pl
from jax.experimental.pallas import tpu as pltpu
from jax.sharding import PartitionSpec as P

LATENT = 512
QK_SCALE = 192 ** -0.5
NORM_EPS = 1e-6
MESH_ID = pl.DeviceIdType.MESH
NUM_DEV = 8
CHUNK = 512
GROUP = 8
HEAD_A, HEAD_B = 16, 9
VMEM_LAYERS = int(8.9 * 2**20)
BF16, F32 = jnp.bfloat16, jnp.float32


def rms_norm(x_rows, gain_vec):
    x_float = x_rows.astype(F32)
    inv_rms = lax.rsqrt(jnp.mean(x_float * x_float, axis=-1, keepdims=True) + NORM_EPS)
    return (x_float * inv_rms * gain_vec).astype(BF16)


def dot(a, b):
    return jnp.dot(a, b, preferred_element_type=F32)


def dot_nt(a, b):
    return lax.dot_general(a, b, (((1,), (1,)), ((), ())), preferred_element_type=F32)


def round_up(n, m):
    return (n + m - 1) // m * m


def head_chunk(i):
    return i + i // HEAD_A * 2


def cuts_of(width):
    return [(lo, min(lo + CHUNK, width)) for lo in range(0, width, CHUNK)]


def layers_kernel(dims, x_hbm, len_hbm, gain_attn_hbm, gain_ffn_hbm, gain_fin_hbm, kv_hbm, wq_hbm, wo_hbm, wg_hbm, wu_hbm, wd_hbm,
                  wh_hbm, rows, buf, x_cur, hrows, qo, outbox, p_buf, ol, ol_send, pr, act, pair_in, total, chip_in,
                  wq_sem, kv_sem, wo_sem, ffn_sem, h_sem, q_sem, o_sem, p_sem, ag_sem, pair_sem, chip_sem, fin_sem, head_sem,
                  len_ref, gain_attn, gain_ffn, gain_fin, in_sem):
    n_layers, n_rows, d_model, n_heads, kv_width, seq_len, width, pad_width, slot_rows, vocab = dims
    half = n_heads // 2
    q_cols = half * kv_width
    n_q, n_d = q_cols // CHUNK, d_model // CHUNK
    o_rows = half * LATENT
    n_t, n_j = round_up(kv_width, 128) // 128, CHUNK // 128
    cuts = cuts_of(width)
    n_vocab = vocab // CHUNK

    me = lax.axis_index('dp')
    core, x_pos, y_pos = me % 2, (me // 2) % 2, me // 4
    flip = lambda c, a, b: ((y_pos + b) % 2) * 4 + ((x_pos + a) % 2) * 2 + (core + c) % 2
    peer = {1: flip(1, 0, 0), 2: flip(0, 1, 0), 4: flip(0, 0, 1), 6: flip(0, 1, 1)}
    other = 1 - core

    def remote(src, dst, sems, dev):
        return pltpu.make_async_remote_copy(src_ref=src, dst_ref=dst, send_sem=sems.at[0], recv_sem=sems.at[1],
                                            device_id={'dp': dev}, device_id_type=MESH_ID)

    wq_at = lambda l, row, n: pl.ds(l % 3 * slot_rows + row, n)
    kv_at = lambda l, row, n: pl.ds((l + 1) % 3 * slot_rows + row, n)
    wo_at = lambda l, row, n: pl.ds((l + 2) % 3 * slot_rows + row, n)
    ffn_at = wq_at

    def wq_copy(l, n):
        cols = pl.ds(pl.multiple_of(core * q_cols + n * CHUNK, 128), CHUNK)
        return pltpu.make_async_copy(wq_hbm.at[l, :, cols], buf.at[wq_at(l, n * d_model, d_model)], wq_sem.at[l, n])

    def kv_copy(l, b):
        row = b * kv_width if isinstance(b, int) else pl.multiple_of(b * kv_width, 64)
        return pltpu.make_async_copy(kv_hbm.at[l, b], buf.at[kv_at(l, row, kv_width)], kv_sem.at[l, b])

    def wo_copy(l, n):
        src = wo_hbm.at[l, pl.ds(pl.multiple_of(core * o_rows, 128), o_rows), pl.ds(n * CHUNK, CHUNK)]
        return pltpu.make_async_copy(src, buf.at[wo_at(l, n * o_rows, o_rows)], wo_sem.at[l, n])

    def ffn_copy(l, i):
        src = (wg_hbm, wu_hbm, wd_hbm)[i // n_d]
        return pltpu.make_async_copy(src.at[l, :, pl.ds((i % n_d) * CHUNK, CHUNK)],
                                     buf.at[ffn_at(l, i * pad_width, width)], ffn_sem.at[l, i])

    def head_copy(i):
        row = head_chunk(i) * d_model
        return pltpu.make_async_copy(wh_hbm.at[:, pl.ds(i * CHUNK, CHUNK)], buf.at[pl.ds(row, d_model)], head_sem.at[i])

    def start(copies):
        for copy in copies:
            copy.start()

    def gather(own, block, sems):
        every, size = [], n_rows // 4
        chunk = lambda ref, c: ref.at[pl.ds(c * size, size)]

        def send(src, j, k):
            copy = remote(src, block(j, k), sems.at[len(every)], peer[k])
            copy.start()
            every.append(copy)
            return copy

        def send_chunk(src, c, j, k):
            copy = remote(chunk(src, c), chunk(block(j, k), c), sems.at[len(every)], peer[k])
            copy.start()
            every.append(copy)
            return copy

        x_order, y_order = (0, 1, 2, 3), (2, 3, 0, 1)
        near = {}
        for cx, cy in zip(x_order, y_order):
            near[2, cx] = send_chunk(own, cx, 0, 2)
            near[4, cy] = send_chunk(own, cy, 0, 4)
        arrivals = [send(own, 0, 1)]
        far = {}
        for i in range(4):
            for j, c in ((2, x_order[i]), (4, y_order[i])):
                near[j, c].wait_recv()
                if i < 2:
                    far[c] = send_chunk(block(j, 0), c, j, 6 - j)
                arrivals.append(send_chunk(block(j, 0), c, j, 1))
        for c in (0, 2, 1, 3):
            far[c].wait_recv()
            arrivals.append(send_chunk(block(6, 0), c, 6, 1))
        for copy in arrivals:
            copy.wait_recv()
        return every

    small = [pltpu.make_async_copy(src, dst, in_sem.at[i]) for i, (src, dst) in enumerate(
        ((x_hbm, x_cur), (gain_attn_hbm, gain_attn), (gain_ffn_hbm, gain_ffn), (gain_fin_hbm, gain_fin), (len_hbm, len_ref)))]
    start(small)
    start(wq_copy(0, n) for n in range(n_q))
    for copy in small:
        copy.wait()

    for l in range(n_layers):
        sent = []
        hrows[0] = rms_norm(x_cur[...], gain_attn[pl.ds(l, 1), :])
        if l == 0:
            barrier = pltpu.get_barrier_semaphore()
            for j in (1, 2, 4, 6):
                pl.semaphore_signal(barrier, inc=1, device_id={'dp': peer[j]}, device_id_type=MESH_ID)
            pl.semaphore_wait(barrier, 4)
        copy = remote(hrows.at[0], hrows.at[1], h_sem.at[l], peer[1])
        copy.start()
        sent.append(copy)
        copy.wait_recv()
        both_rows = hrows[...].reshape(2 * n_rows, d_model)
        prev, q_copies = None, []
        bounds = [(i, min(i + 3, n_q)) for i in range(0, n_q, 3)]
        for first, stop in bounds:
            for n in range(first, stop):
                wq_copy(l, n).wait()
            if l == 0:
                start(kv_copy(l, b) for b in range(first * n_rows // n_q, stop * n_rows // n_q))
            weights = jnp.concatenate([buf[wq_at(l, n * d_model, d_model), :] for n in range(first, stop)], axis=1)
            wide = dot(both_rows, weights).astype(BF16).astype(F32)
            for n in range(first, stop):
                cur = wide[:, (n - first) * CHUNK:(n - first + 1) * CHUNK]
                if n >= 1:
                    h = n - 1
                    off = h * kv_width - h * CHUNK
                    q_head = jnp.concatenate([prev[:, off:], cur[:, :off + kv_width - CHUNK]], axis=1)
                    for j in range(n_t):
                        lanes = slice(j * 128, min((j + 1) * 128, kv_width))
                        keep = pl.ds(0, lanes.stop - lanes.start)
                        at = pl.ds(pl.multiple_of((core * half + h) * n_rows, n_rows), n_rows)
                        qo[j, at, keep] = q_head[:n_rows, lanes]
                        outbox[j, pl.ds(h * n_rows, n_rows), keep] = q_head[n_rows:, lanes]
                    if h % 2:
                        dst = qo.at[:, pl.ds(pl.multiple_of((core * half + h - 1) * n_rows, n_rows), 2 * n_rows)]
                        copy = remote(outbox.at[pl.ds(0, n_t), pl.ds((h - 1) * n_rows, 2 * n_rows)], dst, q_sem.at[l, h // 2], peer[1])
                        copy.start()
                        q_copies.append(copy)
                prev = cur
        if l == 0:
            start(wo_copy(l, n) for n in range(n_d))
        for copy in q_copies:
            copy.wait_recv()

        key_pos = lax.broadcasted_iota(jnp.int32, (n_heads, seq_len), 1)

        def scores(g, l=l):
            slot = lax.rem(g, 2)
            for i in range(GROUP):
                kv_copy(l, g * GROUP + i).wait()
            for i in range(GROUP):
                b = g * GROUP + i
                q = [qo[j, pl.ds(b, n_heads, stride=n_rows), :].astype(BF16) for j in range(n_t)]
                q = jnp.concatenate(q, axis=1)[:, :kv_width]
                row = pl.multiple_of(b * kv_width, 64)
                s = dot(q, buf[kv_at(l, row, kv_width), :]) * QK_SCALE
                s = jnp.where(key_pos < len_ref[0, b], s, -1e30)
                e = jnp.exp(s - jnp.max(s, axis=-1, keepdims=True))
                p_buf[slot, i] = (e / jnp.sum(e, axis=-1, keepdims=True)).astype(BF16)

        def contexts(g, l=l):
            slot = lax.rem(g, 2)
            for i in range(GROUP):
                b = g * GROUP + i
                row = pl.multiple_of(b * kv_width, 64)
                ctx = dot_nt(p_buf[slot, i], buf[kv_at(l, row, LATENT), :])
                for j in range(n_j):
                    qo[j, pl.ds(b, n_heads, stride=n_rows), :] = ctx[:, j * 128:(j + 1) * 128]

        n_groups = n_rows // GROUP
        scores(jnp.int32(0))

        def step(g, carry):
            scores(g)
            contexts(g - 1)
            return carry

        lax.fori_loop(1, n_groups, step, 0)
        contexts(jnp.int32(n_groups - 1))
        if l + 1 == n_layers:
            start(head_copy(i) for i in range(HEAD_A, n_vocab))

        for copy in q_copies:
            copy.wait_send()

        for h in range(half):
            at = pl.ds(pl.multiple_of((other * half + h) * n_rows, n_rows), n_rows)
            for j in range(n_j):
                ol_send[h, :, pl.ds(j * 128, 128)] = qo[j, at, :].astype(BF16)
        o_copy = remote(ol_send, ol.at[1], o_sem.at[l], peer[1])
        o_copy.start()
        sent.append(o_copy)
        start(ffn_copy(l, i) for i in range(3 * n_d))
        for h in range(half):
            at = pl.ds(pl.multiple_of((core * half + h) * n_rows, n_rows), n_rows)
            for j in range(n_j):
                ol[0, h, :, pl.ds(j * 128, 128)] = qo[j, at, :].astype(BF16)
        o_copy.wait_recv()
        p_copies, own = [], []
        context = jnp.concatenate([ol[:, h].reshape(2 * n_rows, LATENT) for h in range(half)], axis=1)
        for first in range(0, n_d, 2):
            for n in (first, first + 1):
                wo_copy(l, n).wait()
            weights = jnp.concatenate([buf[wo_at(l, n * o_rows, o_rows), :] for n in (first, first + 1)], axis=1)
            acc = dot(context, weights)
            for n in (first, first + 1):
                cols = slice((n - first) * CHUNK, (n - first + 1) * CHUNK)
                own.append(acc[:n_rows, cols])
                for j in range(n_j):
                    outbox[n, pl.ds(j * n_rows, n_rows), :] = acc[n_rows:, cols][:, j * 128:(j + 1) * 128]
                copy = remote(outbox.at[n, pl.ds(0, n_j * n_rows)], pr.at[n], p_sem.at[l, n], peer[1])
                copy.start()
                p_copies.append(copy)
        if l + 1 == n_layers:
            start(head_copy(i) for i in range(HEAD_B))
        for n in range(n_d):
            cols = pl.ds(n * CHUNK, CHUNK)
            p_copies[n].wait_recv()
            theirs = jnp.concatenate([pr[n, pl.ds(j * n_rows, n_rows), :] for j in range(n_j)], axis=1)
            x_cur[:, cols] = (x_cur[:, cols].astype(F32) + (own[n] + theirs)).astype(BF16)

        rows[0] = rms_norm(x_cur[...], gain_ffn[pl.ds(l, 1), :])
        row_sends = gather(rows.at[0], lambda j, k: rows.at[j ^ k], ag_sem.at[l])
        if l + 1 < n_layers:
            start(wq_copy(l + 1, n) for n in range(n_q))
        for i in range(2 * n_d):
            ffn_copy(l, i).wait()
        all_rows = rows[...].reshape(NUM_DEV * n_rows, d_model)
        for lo, hi in cuts:
            w_part = [jnp.concatenate([buf[ffn_at(l, (u * n_d + k) * pad_width + lo, hi - lo), :] for k in range(n_d)], axis=1)
                      for u in (0, 1)]
            gate = dot_nt(all_rows, w_part[0])
            up = dot_nt(all_rows, w_part[1])
            act[:, pl.ds(lo, hi - lo)] = (jax.nn.silu(gate) * up).astype(BF16)

        for copy in row_sends + p_copies:
            copy.wait_send()
        pair, chip = [], []

        def reduce_chunk(c):
            pair[c].wait_recv()
            for k in range(4):
                at = pl.ds((c * 4 + k) * n_rows, n_rows)
                for j in range(n_j):
                    lanes = pl.ds(j * 128, 128)
                    both = qo[j, at, :] + pair_in[2 * c + j // 2, pl.ds((j % 2 * 4 + k) * n_rows, n_rows), :]
                    if k == 0:
                        qo[j, at, :] = both
                    else:
                        total[c, k - 1, :, lanes] = both.astype(BF16)
            for k in (3, 1, 2):
                copy = remote(total.at[c, k - 1], chip_in.at[c, k - 1], chip_sem.at[l, c, k - 1], peer[2 * k])
                copy.start()
                chip.append(copy)

        for c in range(n_d):
            ffn_copy(l, 2 * n_d + c).wait()
            y = dot(act[...], buf[ffn_at(l, (2 * n_d + c) * pad_width, width), :])
            y = y.reshape(4, 2, n_rows, CHUNK)
            theirs = y[:, 1].reshape(4 * n_rows, CHUNK)
            for j in range(n_j):
                outbox[2 * c + j // 2, pl.ds(j % 2 * 4 * n_rows, 4 * n_rows), :] = theirs[:, j * 128:(j + 1) * 128]
            mine = y[:, 0].reshape(4 * n_rows, CHUNK)
            for j in range(n_j):
                qo[j, pl.ds(c * 4 * n_rows, 4 * n_rows), :] = mine[:, j * 128:(j + 1) * 128]
            copy = remote(outbox.at[pl.ds(2 * c, 2)], pair_in.at[pl.ds(2 * c, 2)], pair_sem.at[l, c], peer[1])
            copy.start()
            pair.append(copy)
            if c >= 1:
                reduce_chunk(c - 1)
        reduce_chunk(n_d - 1)
        if l + 1 < n_layers:
            start(kv_copy(l + 1, b) for b in range(n_rows))
            start(wo_copy(l + 1, n) for n in range(n_d))
        else:
            start(head_copy(i) for i in range(HEAD_B, HEAD_A))
        for c in range(n_d):
            cols = pl.ds(c * CHUNK, CHUNK)
            for copy in chip[3 * c:3 * c + 3]:
                copy.wait_recv()
            y = jnp.concatenate([qo[j, pl.ds(c * 4 * n_rows, n_rows), :] for j in range(n_j)], axis=1)
            for k in range(3):
                y = y + chip_in[c, k].astype(F32)
            x_cur[:, cols] = (x_cur[:, cols].astype(F32) + y).astype(BF16)
        for copy in sent + pair + chip:
            copy.wait_send()

    hrows[0] = rms_norm(x_cur[...], gain_fin[...])
    rows[me] = hrows[0]
    peer[0] = me
    sends = gather(hrows.at[0], lambda j, k: rows.at[peer[j]], fin_sem)
    for copy in sends:
        copy.wait_send()
    for i in range(n_vocab):
        head_copy(i).wait()


def head_kernel(dims, rows, buf, out_hbm, tile, sem):
    d_model, vocab = dims
    n_vocab = vocab // CHUNK

    def out_copy(i, cols, slot):
        at = pl.ds(i * 2 * CHUNK if isinstance(i, int) else pl.multiple_of(i * 2 * CHUNK, 128), cols)
        return pltpu.make_async_copy(tile.at[slot, :, pl.ds(0, cols)], out_hbm.at[:, at], sem.at[slot])

    def weights(chunk):
        return buf[pl.ds(pl.multiple_of(head_chunk(chunk) * d_model, 128), d_model), :]

    def step(i, carry):
        half = lax.rem(i, 2) * 2

        @pl.when(i >= 2)
        def _():
            for h in (0, 1):
                out_copy(2 * i - 4 + h, 2 * CHUNK, half + h).wait()

        for c in range(4):
            tile[half + c // 2, :, pl.ds(c % 2 * CHUNK, CHUNK)] = dot(x, weights(4 * i + c))
        for h in (0, 1):
            out_copy(2 * i + h, 2 * CHUNK, half + h).start()
        return carry

    x = rows[...].reshape(-1, d_model)
    n_quads = n_vocab // 4
    lax.fori_loop(0, n_quads, step, 0)
    for i in range(max(n_quads - 2, 0), n_quads):
        for h in (0, 1):
            out_copy(2 * i + h, 2 * CHUNK, i % 2 * 2 + h).wait()
        if i == n_quads - 2 and n_vocab % 4:
            last = n_quads % 2 * 2
            tile[last, :, pl.ds(0, CHUNK)] = dot(x, weights(n_vocab - 1))
            out_copy(2 * n_quads, CHUNK, last).start()
    if n_vocab % 4:
        out_copy(2 * n_quads, CHUNK, n_quads % 2 * 2).wait()


def run_head(rows, buf, vocab):
    n_rows, d_model = rows.shape[0] * rows.shape[1], rows.shape[2]
    vmem = pl.BlockSpec(memory_space=pltpu.VMEM)
    rows, buf = (pltpu.with_memory_space_constraint(a, pltpu.VMEM) for a in (rows, buf))
    return pl.pallas_call(
        functools.partial(head_kernel, (d_model, vocab)),
        out_shape=jax.ShapeDtypeStruct((n_rows, vocab), F32),
        in_specs=[vmem, vmem],
        out_specs=pl.BlockSpec(memory_space=pl.ANY),
        scratch_shapes=[pltpu.VMEM((4, n_rows, 2 * CHUNK), F32), pltpu.SemaphoreType.DMA((4,))],
        compiler_params=pltpu.CompilerParams(vmem_limit_bytes=VMEM_LAYERS),
        name='head',
    )(rows, buf)


def run_layers(hidden, lengths, kv_t, gain_attn, w_q, w_o, gain_ffn, wg_t, wu_t, w_down, gain_fin, w_head):
    n_layers, n_rows, kv_width, seq_len = kv_t.shape
    d_model = hidden.shape[1]
    n_heads = w_q.shape[2] // kv_width
    width = w_down.shape[1]
    pad_width = round_up(width, 16)
    half, n_d = n_heads // 2, d_model // CHUNK
    n_q = half * kv_width // CHUNK
    n_t = round_up(kv_width, 128) // 128
    slot_rows = max(n_q * d_model, n_rows * kv_width, n_d * half * LATENT, 3 * n_d * pad_width)
    dims = (n_layers, n_rows, d_model, n_heads, kv_width, seq_len, width, pad_width, slot_rows, w_head.shape[1])
    vmem, anys = pl.BlockSpec(memory_space=pltpu.VMEM), pl.BlockSpec(memory_space=pl.ANY)
    dma = pltpu.SemaphoreType.DMA
    scratch = [
        pltpu.VMEM((n_rows, d_model), BF16),
        pltpu.VMEM((2, n_rows, d_model), BF16),
        pltpu.VMEM((n_t, n_heads * n_rows, 128), F32),
        pltpu.VMEM((8, half * n_rows, 128), F32),
        pltpu.VMEM((2, GROUP, n_heads, seq_len), BF16),
        pltpu.VMEM((2, half, n_rows, LATENT), BF16),
        pltpu.VMEM((half, n_rows, LATENT), BF16),
        pltpu.VMEM((n_d, CHUNK // 128 * n_rows, 128), F32),
        pltpu.VMEM((NUM_DEV * n_rows, width), BF16),
        pltpu.VMEM((8, half * n_rows, 128), F32),
        pltpu.VMEM((n_d, 3, n_rows, CHUNK), BF16),
        pltpu.VMEM((n_d, 3, n_rows, CHUNK), BF16),
        dma((n_layers, n_q)), dma((n_layers, n_rows)), dma((n_layers, n_d)), dma((n_layers, 3 * n_d)),
        dma((n_layers, 2)), dma((n_layers, half // 2, 2)), dma((n_layers, 2)), dma((n_layers, n_d, 2)),
        dma((n_layers, 25, 2)), dma((n_layers, n_d, 2)), dma((n_layers, n_d, 3, 2)), dma((25, 2)), dma((w_head.shape[1] // CHUNK,)),
        pltpu.SMEM((1, n_rows), jnp.int32), pltpu.VMEM((n_layers, d_model), F32), pltpu.VMEM((n_layers, d_model), F32),
        pltpu.VMEM((1, d_model), F32), dma((5,)),
    ]
    return pl.pallas_call(
        functools.partial(layers_kernel, dims),
        out_shape=[pltpu.VMEM((NUM_DEV, n_rows, d_model), BF16), pltpu.VMEM((3 * slot_rows, CHUNK), BF16)],
        in_specs=[anys] * 12,
        out_specs=[vmem, vmem],
        scratch_shapes=scratch,
        compiler_params=pltpu.CompilerParams(collective_id=0, has_side_effects=True, vmem_limit_bytes=VMEM_LAYERS),
        name='layers',
    )(hidden, lengths.reshape(1, -1), gain_attn, gain_ffn, gain_fin.reshape(1, -1), kv_t, w_q, w_o, wg_t, wu_t, w_down, w_head)


def solution(mesh):
    row_axes = ('rep', 'dp')
    specs_in = (P(row_axes, None), P(row_axes), P(None, row_axes, None, None), P(), P(), P(), P(),
                P(None, None, 'dp'), P(None, None, 'dp'), P(None, 'dp', None), P(), P(None, 'dp'))

    def device_step(hidden, lengths, kv_cache, norm_attn, w_q, w_o, norm_ffn, w_gate, w_up, w_down, norm_final, w_head):
        rows, buf = run_layers(hidden, lengths, jnp.swapaxes(kv_cache, 2, 3), norm_attn, w_q, w_o, norm_ffn,
                               jnp.swapaxes(w_gate, 1, 2), jnp.swapaxes(w_up, 1, 2), w_down, norm_final, w_head)
        return run_head(rows, buf, w_head.shape[1])

    return jax.shard_map(device_step, mesh=mesh, in_specs=specs_in, out_specs=P('rep', 'dp'), check_vma=False)
```

```python
import functools

import jax
import jax.numpy as jnp
from jax import lax
from jax.experimental import pallas as pl
from jax.experimental.pallas import tpu as pltpu
from jax.sharding import PartitionSpec as P

LATENT = 512
QK_SCALE = 192 ** -0.5
NORM_EPS = 1e-6
MESH_ID = pl.DeviceIdType.MESH
NUM_DEV = 8
CHUNK = 512
GROUP = 8
HEAD_A, HEAD_B = 16, 9
VMEM_LAYERS = int(8.9 * 2**20)
BF16, F32 = jnp.bfloat16, jnp.float32


def rms_norm(x_rows, gain_vec):
    x_float = x_rows.astype(F32)
    inv_rms = lax.rsqrt(jnp.mean(x_float * x_float, axis=-1, keepdims=True) + NORM_EPS)
    return (x_float * inv_rms * gain_vec).astype(BF16)


def dot(a, b):
    return jnp.dot(a, b, preferred_element_type=F32)


def dot_nt(a, b):
    return lax.dot_general(a, b, (((1,), (1,)), ((), ())), preferred_element_type=F32)


def round_up(n, m):
    return (n + m - 1) // m * m


def head_chunk(i):
    return i + i // HEAD_A * 2


def cuts_of(width):
    return [(lo, min(lo + CHUNK, width)) for lo in range(0, width, CHUNK)]


def layers_kernel(dims, x_ref, len_ref, gain_attn, gain_ffn, gain_fin, kv_hbm, wq_hbm, wo_hbm, wg_hbm, wu_hbm, wd_hbm,
                  wh_hbm, rows, buf, x_cur, hrows, qo, outbox, p_buf, ol, ol_send, pr, act, pair_in, total, chip_in,
                  wq_sem, kv_sem, wo_sem, ffn_sem, h_sem, q_sem, o_sem, p_sem, ag_sem, pair_sem, chip_sem, fin_sem, head_sem):
    n_layers, n_rows, d_model, n_heads, kv_width, seq_len, width, pad_width, slot_rows, vocab = dims
    half = n_heads // 2
    q_cols = half * kv_width
    n_q, n_d = q_cols // CHUNK, d_model // CHUNK
    o_rows = half * LATENT
    n_t, n_j = round_up(kv_width, 128) // 128, CHUNK // 128
    cuts = cuts_of(width)
    n_vocab = vocab // CHUNK

    me = lax.axis_index('dp')
    core, x_pos, y_pos = me % 2, (me // 2) % 2, me // 4
    flip = lambda c, a, b: ((y_pos + b) % 2) * 4 + ((x_pos + a) % 2) * 2 + (core + c) % 2
    peer = {1: flip(1, 0, 0), 2: flip(0, 1, 0), 4: flip(0, 0, 1), 6: flip(0, 1, 1)}
    other = 1 - core

    def remote(src, dst, sems, dev):
        return pltpu.make_async_remote_copy(src_ref=src, dst_ref=dst, send_sem=sems.at[0], recv_sem=sems.at[1],
                                            device_id={'dp': dev}, device_id_type=MESH_ID)

    wq_at = lambda l, row, n: pl.ds(l % 3 * slot_rows + row, n)
    kv_at = lambda l, row, n: pl.ds((l + 1) % 3 * slot_rows + row, n)
    wo_at = lambda l, row, n: pl.ds((l + 2) % 3 * slot_rows + row, n)
    ffn_at = wq_at

    def wq_copy(l, n):
        cols = pl.ds(pl.multiple_of(core * q_cols + n * CHUNK, 128), CHUNK)
        return pltpu.make_async_copy(wq_hbm.at[l, :, cols], buf.at[wq_at(l, n * d_model, d_model)], wq_sem.at[l, n])

    def kv_copy(l, b):
        row = b * kv_width if isinstance(b, int) else pl.multiple_of(b * kv_width, 64)
        return pltpu.make_async_copy(kv_hbm.at[l, b], buf.at[kv_at(l, row, kv_width)], kv_sem.at[l, b])

    def wo_copy(l, n):
        src = wo_hbm.at[l, pl.ds(pl.multiple_of(core * o_rows, 128), o_rows), pl.ds(n * CHUNK, CHUNK)]
        return pltpu.make_async_copy(src, buf.at[wo_at(l, n * o_rows, o_rows)], wo_sem.at[l, n])

    def ffn_copy(l, i):
        src = (wg_hbm, wu_hbm, wd_hbm)[i // n_d]
        return pltpu.make_async_copy(src.at[l, :, pl.ds((i % n_d) * CHUNK, CHUNK)],
                                     buf.at[ffn_at(l, i * pad_width, width)], ffn_sem.at[l, i])

    def head_copy(i):
        row = head_chunk(i) * d_model
        return pltpu.make_async_copy(wh_hbm.at[:, pl.ds(i * CHUNK, CHUNK)], buf.at[pl.ds(row, d_model)], head_sem.at[i])

    def start(copies):
        for copy in copies:
            copy.start()

    def gather(own, block, sems):
        every, size = [], n_rows // 4
        chunk = lambda ref, c: ref.at[pl.ds(c * size, size)]

        def send(src, j, k):
            copy = remote(src, block(j, k), sems.at[len(every)], peer[k])
            copy.start()
            every.append(copy)
            return copy

        def send_chunk(src, c, j, k):
            copy = remote(chunk(src, c), chunk(block(j, k), c), sems.at[len(every)], peer[k])
            copy.start()
            every.append(copy)
            return copy

        x_order, y_order = (0, 1, 2, 3), (2, 3, 0, 1)
        near = {}
        for cx, cy in zip(x_order, y_order):
            near[2, cx] = send_chunk(own, cx, 0, 2)
            near[4, cy] = send_chunk(own, cy, 0, 4)
        arrivals = [send(own, 0, 1)]
        far = {}
        for i in range(4):
            for j, c in ((2, x_order[i]), (4, y_order[i])):
                near[j, c].wait_recv()
                if i < 2:
                    far[c] = send_chunk(block(j, 0), c, j, 6 - j)
                arrivals.append(send_chunk(block(j, 0), c, j, 1))
        for c in (0, 2, 1, 3):
            far[c].wait_recv()
            arrivals.append(send_chunk(block(6, 0), c, 6, 1))
        for copy in arrivals:
            copy.wait_recv()
        return every

    start(wq_copy(0, n) for n in range(n_q))
    x_cur[...] = x_ref[...]

    for l in range(n_layers):
        sent = []
        hrows[0] = rms_norm(x_cur[...], gain_attn[pl.ds(l, 1), :])
        if l == 0:
            barrier = pltpu.get_barrier_semaphore()
            for j in (1, 2, 4, 6):
                pl.semaphore_signal(barrier, inc=1, device_id={'dp': peer[j]}, device_id_type=MESH_ID)
            pl.semaphore_wait(barrier, 4)
        copy = remote(hrows.at[0], hrows.at[1], h_sem.at[l], peer[1])
        copy.start()
        sent.append(copy)
        copy.wait_recv()
        both_rows = hrows[...].reshape(2 * n_rows, d_model)
        prev, q_copies = None, []
        bounds = [(i, min(i + 3, n_q)) for i in range(0, n_q, 3)]
        if l == 0:
            bounds[-1:] = [(n_q - 3, n_q - 1), (n_q - 1, n_q)]
        for first, stop in bounds:
            for n in range(first, stop):
                wq_copy(l, n).wait()
            if l == 0:
                start(kv_copy(l, b) for b in range(first * n_rows // n_q, stop * n_rows // n_q))
            weights = jnp.concatenate([buf[wq_at(l, n * d_model, d_model), :] for n in range(first, stop)], axis=1)
            wide = dot(both_rows, weights).astype(BF16).astype(F32)
            for n in range(first, stop):
                cur = wide[:, (n - first) * CHUNK:(n - first + 1) * CHUNK]
                if n >= 1:
                    h = n - 1
                    off = h * kv_width - h * CHUNK
                    q_head = jnp.concatenate([prev[:, off:], cur[:, :off + kv_width - CHUNK]], axis=1)
                    for j in range(n_t):
                        lanes = slice(j * 128, min((j + 1) * 128, kv_width))
                        keep = pl.ds(0, lanes.stop - lanes.start)
                        at = pl.ds(pl.multiple_of((core * half + h) * n_rows, n_rows), n_rows)
                        qo[j, at, keep] = q_head[:n_rows, lanes]
                        outbox[j, pl.ds(h * n_rows, n_rows), keep] = q_head[n_rows:, lanes]
                    if h % 2:
                        dst = qo.at[:, pl.ds(pl.multiple_of((core * half + h - 1) * n_rows, n_rows), 2 * n_rows)]
                        copy = remote(outbox.at[pl.ds(0, n_t), pl.ds((h - 1) * n_rows, 2 * n_rows)], dst, q_sem.at[l, h // 2], peer[1])
                        copy.start()
                        q_copies.append(copy)
                prev = cur
        if l == 0:
            start(wo_copy(l, n) for n in range(n_d))
        for copy in q_copies:
            copy.wait_recv()

        key_pos = lax.broadcasted_iota(jnp.int32, (n_heads, seq_len), 1)

        def scores(g, l=l):
            slot = lax.rem(g, 2)
            for i in range(GROUP):
                kv_copy(l, g * GROUP + i).wait()
            for i in range(GROUP):
                b = g * GROUP + i
                q = [qo[j, pl.ds(b, n_heads, stride=n_rows), :].astype(BF16) for j in range(n_t)]
                q = jnp.concatenate(q, axis=1)[:, :kv_width]
                row = pl.multiple_of(b * kv_width, 64)
                s = dot(q, buf[kv_at(l, row, kv_width), :]) * QK_SCALE
                s = jnp.where(key_pos < len_ref[b], s, -1e30)
                e = jnp.exp(s - jnp.max(s, axis=-1, keepdims=True))
                p_buf[slot, i] = (e / jnp.sum(e, axis=-1, keepdims=True)).astype(BF16)

        def contexts(g, l=l):
            slot = lax.rem(g, 2)
            for i in range(GROUP):
                b = g * GROUP + i
                row = pl.multiple_of(b * kv_width, 64)
                ctx = dot_nt(p_buf[slot, i], buf[kv_at(l, row, LATENT), :])
                for j in range(n_j):
                    qo[j, pl.ds(b, n_heads, stride=n_rows), :] = ctx[:, j * 128:(j + 1) * 128]

        n_groups = n_rows // GROUP
        scores(jnp.int32(0))

        def step(g, carry):
            scores(g)
            contexts(g - 1)
            return carry

        lax.fori_loop(1, n_groups, step, 0)
        contexts(jnp.int32(n_groups - 1))
        if l + 1 == n_layers:
            start(head_copy(i) for i in range(HEAD_A, n_vocab))

        for copy in q_copies:
            copy.wait_send()

        for h in range(half):
            at = pl.ds(pl.multiple_of((other * half + h) * n_rows, n_rows), n_rows)
            for j in range(n_j):
                ol_send[h, :, pl.ds(j * 128, 128)] = qo[j, at, :].astype(BF16)
        o_copy = remote(ol_send, ol.at[1], o_sem.at[l], peer[1])
        o_copy.start()
        sent.append(o_copy)
        start(ffn_copy(l, i) for i in range(3 * n_d))
        for h in range(half):
            at = pl.ds(pl.multiple_of((core * half + h) * n_rows, n_rows), n_rows)
            for j in range(n_j):
                ol[0, h, :, pl.ds(j * 128, 128)] = qo[j, at, :].astype(BF16)
        o_copy.wait_recv()
        p_copies, own = [], []
        context = jnp.concatenate([ol[:, h].reshape(2 * n_rows, LATENT) for h in range(half)], axis=1)
        for first in range(0, n_d, 2):
            for n in (first, first + 1):
                wo_copy(l, n).wait()
            weights = jnp.concatenate([buf[wo_at(l, n * o_rows, o_rows), :] for n in (first, first + 1)], axis=1)
            acc = dot(context, weights)
            for n in (first, first + 1):
                cols = slice((n - first) * CHUNK, (n - first + 1) * CHUNK)
                own.append(acc[:n_rows, cols])
                for j in range(n_j):
                    outbox[n, pl.ds(j * n_rows, n_rows), :] = acc[n_rows:, cols][:, j * 128:(j + 1) * 128]
                copy = remote(outbox.at[n, pl.ds(0, n_j * n_rows)], pr.at[n], p_sem.at[l, n], peer[1])
                copy.start()
                p_copies.append(copy)
        if l + 1 == n_layers:
            start(head_copy(i) for i in range(HEAD_B))
        for n in range(n_d):
            cols = pl.ds(n * CHUNK, CHUNK)
            p_copies[n].wait_recv()
            theirs = jnp.concatenate([pr[n, pl.ds(j * n_rows, n_rows), :] for j in range(n_j)], axis=1)
            x_cur[:, cols] = (x_cur[:, cols].astype(F32) + (own[n] + theirs)).astype(BF16)

        rows[0] = rms_norm(x_cur[...], gain_ffn[pl.ds(l, 1), :])
        row_sends = gather(rows.at[0], lambda j, k: rows.at[j ^ k], ag_sem.at[l])
        if l + 1 < n_layers:
            start(wq_copy(l + 1, n) for n in range(n_q))
        for i in range(2 * n_d):
            ffn_copy(l, i).wait()
        all_rows = rows[...].reshape(NUM_DEV * n_rows, d_model)
        for lo, hi in cuts:
            w_part = [jnp.concatenate([buf[ffn_at(l, (u * n_d + k) * pad_width + lo, hi - lo), :] for k in range(n_d)], axis=1)
                      for u in (0, 1)]
            gate = dot_nt(all_rows, w_part[0])
            up = dot_nt(all_rows, w_part[1])
            act[:, pl.ds(lo, hi - lo)] = (jax.nn.silu(gate) * up).astype(BF16)

        for copy in row_sends + p_copies:
            copy.wait_send()
        pair, chip = [], []

        def reduce_chunk(c):
            pair[c].wait_recv()
            for k in range(4):
                at = pl.ds((c * 4 + k) * n_rows, n_rows)
                for j in range(n_j):
                    lanes = pl.ds(j * 128, 128)
                    both = qo[j, at, :] + pair_in[2 * c + j // 2, pl.ds((j % 2 * 4 + k) * n_rows, n_rows), :]
                    if k == 0:
                        qo[j, at, :] = both
                    else:
                        total[c, k - 1, :, lanes] = both.astype(BF16)
            for k in (3, 1, 2):
                copy = remote(total.at[c, k - 1], chip_in.at[c, k - 1], chip_sem.at[l, c, k - 1], peer[2 * k])
                copy.start()
                chip.append(copy)

        for c in range(n_d):
            ffn_copy(l, 2 * n_d + c).wait()
            y = dot(act[...], buf[ffn_at(l, (2 * n_d + c) * pad_width, width), :])
            y = y.reshape(4, 2, n_rows, CHUNK)
            theirs = y[:, 1].reshape(4 * n_rows, CHUNK)
            for j in range(n_j):
                outbox[2 * c + j // 2, pl.ds(j % 2 * 4 * n_rows, 4 * n_rows), :] = theirs[:, j * 128:(j + 1) * 128]
            mine = y[:, 0].reshape(4 * n_rows, CHUNK)
            for j in range(n_j):
                qo[j, pl.ds(c * 4 * n_rows, 4 * n_rows), :] = mine[:, j * 128:(j + 1) * 128]
            copy = remote(outbox.at[pl.ds(2 * c, 2)], pair_in.at[pl.ds(2 * c, 2)], pair_sem.at[l, c], peer[1])
            copy.start()
            pair.append(copy)
            if c >= 1:
                reduce_chunk(c - 1)
        reduce_chunk(n_d - 1)
        if l + 1 < n_layers:
            start(kv_copy(l + 1, b) for b in range(n_rows))
            start(wo_copy(l + 1, n) for n in range(n_d))
        else:
            start(head_copy(i) for i in range(HEAD_B, HEAD_A))
        for c in range(n_d):
            cols = pl.ds(c * CHUNK, CHUNK)
            for copy in chip[3 * c:3 * c + 3]:
                copy.wait_recv()
            y = jnp.concatenate([qo[j, pl.ds(c * 4 * n_rows, n_rows), :] for j in range(n_j)], axis=1)
            for k in range(3):
                y = y + chip_in[c, k].astype(F32)
            x_cur[:, cols] = (x_cur[:, cols].astype(F32) + y).astype(BF16)
        for copy in sent + pair + chip:
            copy.wait_send()

    hrows[0] = rms_norm(x_cur[...], gain_fin[...])
    rows[me] = hrows[0]
    peer[0] = me
    sends = gather(hrows.at[0], lambda j, k: rows.at[peer[j]], fin_sem)
    for copy in sends:
        copy.wait_send()
    for i in range(n_vocab):
        head_copy(i).wait()


def head_kernel(dims, rows, buf, out_hbm, tile, sem):
    d_model, vocab = dims
    n_vocab = vocab // CHUNK

    def out_copy(i, cols, slot):
        at = pl.ds(i * 2 * CHUNK if isinstance(i, int) else pl.multiple_of(i * 2 * CHUNK, 128), cols)
        return pltpu.make_async_copy(tile.at[slot, :, pl.ds(0, cols)], out_hbm.at[:, at], sem.at[slot])

    def weights(chunk):
        return buf[pl.ds(pl.multiple_of(head_chunk(chunk) * d_model, 128), d_model), :]

    def step(i, carry):
        half = lax.rem(i, 2) * 2

        @pl.when(i >= 2)
        def _():
            for h in (0, 1):
                out_copy(2 * i - 4 + h, 2 * CHUNK, half + h).wait()

        for c in range(4):
            tile[half + c // 2, :, pl.ds(c % 2 * CHUNK, CHUNK)] = dot(x, weights(4 * i + c))
        for h in (0, 1):
            out_copy(2 * i + h, 2 * CHUNK, half + h).start()
        return carry

    x = rows[...].reshape(-1, d_model)
    n_quads = n_vocab // 4
    lax.fori_loop(0, n_quads, step, 0)
    for i in range(max(n_quads - 2, 0), n_quads):
        for h in (0, 1):
            out_copy(2 * i + h, 2 * CHUNK, i % 2 * 2 + h).wait()
        if i == n_quads - 2 and n_vocab % 4:
            last = n_quads % 2 * 2
            tile[last, :, pl.ds(0, CHUNK)] = dot(x, weights(n_vocab - 1))
            out_copy(2 * n_quads, CHUNK, last).start()
    if n_vocab % 4:
        out_copy(2 * n_quads, CHUNK, n_quads % 2 * 2).wait()


def run_head(rows, buf, vocab):
    n_rows, d_model = rows.shape[0] * rows.shape[1], rows.shape[2]
    vmem = pl.BlockSpec(memory_space=pltpu.VMEM)
    rows, buf = (pltpu.with_memory_space_constraint(a, pltpu.VMEM) for a in (rows, buf))
    return pl.pallas_call(
        functools.partial(head_kernel, (d_model, vocab)),
        out_shape=jax.ShapeDtypeStruct((n_rows, vocab), F32),
        in_specs=[vmem, vmem],
        out_specs=pl.BlockSpec(memory_space=pl.ANY),
        scratch_shapes=[pltpu.VMEM((4, n_rows, 2 * CHUNK), F32), pltpu.SemaphoreType.DMA((4,))],
        compiler_params=pltpu.CompilerParams(vmem_limit_bytes=VMEM_LAYERS),
        name='head',
    )(rows, buf)


def run_layers(hidden, lengths, kv_t, gain_attn, w_q, w_o, gain_ffn, wg_t, wu_t, w_down, gain_fin, w_head):
    n_layers, n_rows, kv_width, seq_len = kv_t.shape
    d_model = hidden.shape[1]
    n_heads = w_q.shape[2] // kv_width
    width = w_down.shape[1]
    pad_width = round_up(width, 16)
    half, n_d = n_heads // 2, d_model // CHUNK
    n_q = half * kv_width // CHUNK
    n_t = round_up(kv_width, 128) // 128
    slot_rows = max(n_q * d_model, n_rows * kv_width, n_d * half * LATENT, 3 * n_d * pad_width)
    dims = (n_layers, n_rows, d_model, n_heads, kv_width, seq_len, width, pad_width, slot_rows, w_head.shape[1])
    vmem, anys = pl.BlockSpec(memory_space=pltpu.VMEM), pl.BlockSpec(memory_space=pl.ANY)
    smem = pl.BlockSpec(memory_space=pltpu.SMEM)
    dma = pltpu.SemaphoreType.DMA
    scratch = [
        pltpu.VMEM((n_rows, d_model), BF16),
        pltpu.VMEM((2, n_rows, d_model), BF16),
        pltpu.VMEM((n_t, n_heads * n_rows, 128), F32),
        pltpu.VMEM((8, half * n_rows, 128), F32),
        pltpu.VMEM((2, GROUP, n_heads, seq_len), BF16),
        pltpu.VMEM((2, half, n_rows, LATENT), BF16),
        pltpu.VMEM((half, n_rows, LATENT), BF16),
        pltpu.VMEM((n_d, CHUNK // 128 * n_rows, 128), F32),
        pltpu.VMEM((NUM_DEV * n_rows, width), BF16),
        pltpu.VMEM((8, half * n_rows, 128), F32),
        pltpu.VMEM((n_d, 3, n_rows, CHUNK), BF16),
        pltpu.VMEM((n_d, 3, n_rows, CHUNK), BF16),
        dma((n_layers, n_q)), dma((n_layers, n_rows)), dma((n_layers, n_d)), dma((n_layers, 3 * n_d)),
        dma((n_layers, 2)), dma((n_layers, half // 2, 2)), dma((n_layers, 2)), dma((n_layers, n_d, 2)),
        dma((n_layers, 25, 2)), dma((n_layers, n_d, 2)), dma((n_layers, n_d, 3, 2)), dma((25, 2)), dma((w_head.shape[1] // CHUNK,)),
    ]
    return pl.pallas_call(
        functools.partial(layers_kernel, dims),
        out_shape=[pltpu.VMEM((NUM_DEV, n_rows, d_model), BF16), pltpu.VMEM((3 * slot_rows, CHUNK), BF16)],
        in_specs=[vmem, smem, vmem, vmem, vmem] + [anys] * 7,
        out_specs=[vmem, vmem],
        scratch_shapes=scratch,
        compiler_params=pltpu.CompilerParams(collective_id=0, has_side_effects=True, vmem_limit_bytes=VMEM_LAYERS),
        name='layers',
    )(hidden, lengths, gain_attn, gain_ffn, gain_fin.reshape(1, -1), kv_t, w_q, w_o, wg_t, wu_t, w_down, w_head)


def solution(mesh):
    row_axes = ('rep', 'dp')
    specs_in = (P(row_axes, None), P(row_axes), P(None, row_axes, None, None), P(), P(), P(), P(),
                P(None, None, 'dp'), P(None, None, 'dp'), P(None, 'dp', None), P(), P(None, 'dp'))

    def device_step(hidden, lengths, kv_cache, norm_attn, w_q, w_o, norm_ffn, w_gate, w_up, w_down, norm_final, w_head):
        rows, buf = run_layers(hidden, lengths, jnp.swapaxes(kv_cache, 2, 3), norm_attn, w_q, w_o, norm_ffn,
                               jnp.swapaxes(w_gate, 1, 2), jnp.swapaxes(w_up, 1, 2), w_down, norm_final, w_head)
        return run_head(rows, buf, w_head.shape[1])

    return jax.shard_map(device_step, mesh=mesh, in_specs=specs_in, out_specs=P('rep', 'dp'), check_vma=False)
```
